128 devices in a mesh: sim: 32 (over z, y, x_hi), learn: 4 (over x_lo, core).
Axes of the slice: x: 4 (x_hi: 2, x_lo: 2; x = x_hi * 2 + x_lo), y: 4, z: 4, core: 2. Of those that a mesh axis runs over, the one named last changes fastest.
Arguments:
- state_field: float32 [128, 512, 2048], P(None, 'sim', 'learn'), may hold values from -6 to 6
- diffusion: float32 [128], replicated, may hold values from 0.03 to 0.24
- weight_in: float32 [128, 1024], replicated, may hold values from -0.5 to 0.5
- weight_mid: float32 [1024, 1024], replicated, may hold values from -0.1875 to 0.1875
- weight_out: float32 [1024, 128], replicated, may hold values from -0.1875 to 0.1875
- block_tile: int32 [1536, 1], P('learn'), may hold values from 0 to 31; in each aligned block of 12 rows (0 to 11, 12 to 23, ...) no two rows name the same one
- block_pos: int32 [1536], P('learn'), may hold values from 0 to 63
Outputs:
- new_state: float32 [128, 512, 2048], P(None, 'sim', 'learn')
- new_in: float32 [128, 1024], replicated
- new_mid: float32 [1024, 1024], replicated
- new_out: float32 [1024, 128], replicated
The draws below stay inside these ranges and needn't reach their ends.
Inputs may be any that keep to these rules, and one draw needn't show every extreme that they name: `block_tile`: in each aligned block of 12 rows no tile index appears twice.
All inputs are finite; a program needn't handle non-finite values.
Results may differ from the reference program's by a relative error of at most 0.0003.
The reference program's roundings to bfloat16 on the way (of `inputs`, `targets` and `error`) count: a program that leaves them out, or rounds other values in their place, can miss the bound.
Values may be sent and summed in bfloat16 or wider, within the bound.
No kernel may reach another device: no remote copies, remote signals or barrier semaphores. Data moves between devices by JAX's collectives and lax.ppermute only.
A program may use at most 128 MiB of HBM per device.

```python
import math
import jax
import jax.numpy as jnp
import numpy as np
from jax import lax

LEV = 128
HID = 1024
BW = 128
RY = 16
RX = 512
SAMPLES = 12
NY = 512
NX = 2048
REQ = 1536
N_SIM = 32


def place_ends(result, stream_key, least, largest):
    extent = result.shape
    place = [jax.random.randint(jax.random.fold_in(stream_key, axis), (), 0, extent[axis]) for axis in range(len(extent))]
    result = result.at[tuple(place)].set(least)
    longest = extent.index(max(extent))
    place[longest] = (place[longest] + 1) % extent[longest]
    return result.at[tuple(place)].set(largest)


def levels(stream_key, shape, cuts, low, top_value):
    level = 1.0
    for axis_at, parts in cuts:
        heights = jax.random.uniform(jax.random.fold_in(jax.random.fold_in(stream_key, 6), axis_at), (parts,), jnp.float32, low / len(cuts), top_value / len(cuts))
        level = level * jnp.repeat(jnp.exp(heights), shape[axis_at] // parts).reshape((-1,) + (1,) * (len(shape) - 1 - axis_at))
    return level


def deal_out(rng, own, number, rows, number_of, top, bound, slope):
    sequence = jax.random.permutation(rng, number_of)
    crowded, ordinary = load_shares(number_of, rows * top, bound, slope, True), load_shares(number_of, rows * top, bound, slope, False)
    places = jnp.arange(number_of)

    def named(sizes, rotation):
        used = int((sizes > 0).sum())
        fixed = max(1, used // 4)
        passed = fixed + (places - fixed + rotation * (used - fixed)) % max(1, number_of - fixed)
        return jnp.zeros((number_of,), jnp.int32).at[sequence[jnp.where(places < fixed, places, passed)]].set(jnp.asarray(sizes, jnp.int32))

    sizes = jnp.where(number % 4 == 0, named(crowded, number // 4), named(ordinary, number - number // 4 - 1))
    mixed = jax.random.permutation(jax.random.fold_in(own, 3), number_of)
    source_of, receiver = mixed[0:number_of // 2 * 2:2], mixed[1:number_of // 2 * 2:2]
    room = jnp.minimum(sizes[source_of] - 1, bound - sizes[receiver]) // 2
    room = jnp.where((source_of == sequence[0]) | (receiver == sequence[0]) | (sizes[receiver] == 0), 0, jnp.maximum(room, 0))
    passed = jax.random.randint(jax.random.fold_in(own, 4), (number_of // 2,), 0, 1 << 20) % (room + 1)
    sizes = sizes.at[source_of].add(-passed).at[receiver].add(passed)
    labels = jnp.searchsorted(jnp.cumsum(sizes), jnp.arange(rows * top), side="right").astype(jnp.int32)
    table = labels.reshape(top, rows).T
    table = table[jax.random.permutation(jax.random.fold_in(own, 1), rows)]
    rotation = jax.random.randint(jax.random.fold_in(own, 2), (rows, 1), 0, top)
    return jnp.take_along_axis(table, (jnp.arange(top)[None, :] + rotation) % top, axis=1)


def load_shares(amount, total, bound, skew, full):
    loads = [(1 << 20) // math.isqrt(rank ** skew) + 1 for rank in range(1, amount + 1)]
    largest = bound if full else min(bound, max(-(-total // amount), total * loads[0] // sum(loads)))
    least = 1 if total - largest >= amount - 1 else 0
    holding, spare = [largest] + [least] * (amount - 1), total - largest - least * (amount - 1)
    while spare > 0:
        candidates = [i for i in range(1, amount) if holding[i] < largest] or [i for i in range(1, amount) if holding[i] < bound]
        whole, left = sum([loads[i] for i in candidates]), spare
        for i in candidates:
            addition = min(bound - holding[i], max(1, left * loads[i] // whole), spare)
            holding[i] = holding[i] + addition
            spare = spare - addition
    return np.array(holding)


def centred(stream_key, dims, scale, limit, shards=(), kind=jnp.bfloat16):
    array = scale * jax.random.normal(stream_key, dims, jnp.float32)
    if shards:
        array = array * levels(stream_key, dims, shards, -0.22, 0.18)
    return jnp.clip(array, -limit, limit).astype(kind)


def setup_inputs(seed: int = 0) -> dict:
    splits = jax.random.split(jax.random.key(seed), 8)
    state_field = centred(splits[0], (LEV, NY, NX), 1.0, 6.0, ((1, 32), (2, 4)), jnp.float32)
    diffusion = jnp.clip(jnp.exp(jax.random.uniform(splits[1], (LEV,), jnp.float32, math.log(0.03), math.log(0.24))), 0.03, 0.24)
    weight_in = centred(splits[2], (LEV, HID), LEV ** -0.5, 0.5, (), jnp.float32)
    weight_mid = centred(splits[3], (HID, HID), HID ** -0.5, 0.1875, (), jnp.float32)
    weight_out = centred(splits[4], (HID, LEV), HID ** -0.5, 0.1875, (), jnp.float32)
    block_tile_keys = jax.random.split(jax.random.fold_in(splits[5], 1), REQ // SAMPLES)
    block_tile_turns = jax.random.permutation(jax.random.fold_in(splits[5], 3), REQ // SAMPLES)
    block_tile = jax.vmap(lambda own, number: deal_out(jax.random.fold_in(splits[5], 2), own, number, SAMPLES, N_SIM, 1, 1, 2))(block_tile_keys, block_tile_turns).reshape((REQ, 1))
    block_pos = place_ends(jax.random.randint(splits[6], (REQ,), 0, RY * (RX // BW)), jax.random.fold_in(splits[6], 1), 0, (RY * (RX // BW)) - 1).astype(jnp.int32)
    return dict(state_field=state_field, diffusion=diffusion, weight_in=weight_in, weight_mid=weight_mid, weight_out=weight_out, block_tile=block_tile, block_pos=block_pos)


RATE = 0.5
TARGET_GAIN = 4.0


def diffuse_once(field, diffusion):
    beside_all = jnp.roll(field, 1, 1) + jnp.roll(field, -1, 1)
    beside_all = beside_all + jnp.roll(field, 1, 2) + jnp.roll(field, -1, 2)
    return field + diffusion[:, None, None] * (beside_all - 4.0 * field)


def silu_slope(value):
    sigma = jax.nn.sigmoid(value)
    return sigma * (1.0 + value * (1.0 - sigma))


def gradients(inputs, targets, weight_in, weight_mid, weight_out, count):
    first = weight_in.astype(jnp.bfloat16)
    second = weight_mid.astype(jnp.bfloat16)
    third = weight_out.astype(jnp.bfloat16)
    pre_one = jnp.dot(inputs, first, preferred_element_type=jnp.float32)
    act_one = jax.nn.silu(pre_one).astype(jnp.bfloat16)
    pre_two = jnp.dot(act_one, second, preferred_element_type=jnp.float32)
    act_two = jax.nn.silu(pre_two).astype(jnp.bfloat16)
    output = jnp.dot(act_two, third, preferred_element_type=jnp.float32)
    error = ((output - targets.astype(jnp.float32)) / count).astype(jnp.bfloat16)
    grad_out = jnp.dot(act_two.T, error, preferred_element_type=jnp.float32)
    back_two = jnp.dot(error, third.T, preferred_element_type=jnp.float32)
    delta_two = (back_two * silu_slope(pre_two)).astype(jnp.bfloat16)
    grad_mid = jnp.dot(act_one.T, delta_two, preferred_element_type=jnp.float32)
    back_one = jnp.dot(delta_two, second.T, preferred_element_type=jnp.float32)
    delta_one = (back_one * silu_slope(pre_one)).astype(jnp.bfloat16)
    grad_in = jnp.dot(inputs.T, delta_one, preferred_element_type=jnp.float32)
    return grad_in, grad_mid, grad_out


def reference(state_field, diffusion, weight_in, weight_mid, weight_out, block_tile, block_pos):
    after = diffuse_once(diffuse_once(state_field, diffusion), diffusion)
    increment = after - state_field
    per_row = RX // BW
    total = block_tile.shape[0]
    request = jnp.arange(total, dtype=jnp.int32)
    learner = request // (N_SIM * SAMPLES)
    owner = block_tile[:, 0].astype(jnp.int32)
    places = block_pos.astype(jnp.int32)
    row_start = (owner * RY + places // per_row).astype(jnp.int32)
    col_start = (learner * RX + (places % per_row) * BW).astype(jnp.int32)

    def cut(row, start):
        zero = jnp.zeros((), jnp.int32)
        piece_in = lax.dynamic_slice(state_field, (zero, row, start), (LEV, 1, BW))[:, 0, :]
        piece_target = lax.dynamic_slice(increment, (zero, row, start), (LEV, 1, BW))[:, 0, :]
        return piece_in, piece_target

    cols_in, cols_target = jax.vmap(cut)(row_start, col_start)
    inputs = jnp.swapaxes(cols_in, 1, 2).astype(jnp.bfloat16)
    targets = (TARGET_GAIN * jnp.swapaxes(cols_target, 1, 2)).astype(jnp.bfloat16)
    groups = total // SAMPLES
    inputs = inputs.reshape(groups, SAMPLES * BW, LEV)
    targets = targets.reshape(groups, SAMPLES * BW, LEV)
    count = float(total * BW)

    def accumulate(carry, pair):
        terms = gradients(pair[0], pair[1], weight_in, weight_mid, weight_out, count)
        return tuple(c + t for c, t in zip(carry, terms)), None

    start = (jnp.zeros((LEV, HID), jnp.float32), jnp.zeros((HID, HID), jnp.float32), jnp.zeros((HID, LEV), jnp.float32))
    sums, _ = lax.scan(accumulate, start, (inputs, targets))
    return (after, weight_in - RATE * sums[0], weight_mid - RATE * sums[1], weight_out - RATE * sums[2])
```

```python
import functools
import math

import jax
import jax.numpy as jnp
from jax import lax
from jax.experimental import pallas as pl
from jax.experimental.pallas import tpu as pltpu
from jax.sharding import Mesh
from jax.sharding import PartitionSpec as P

BW = 128
RATE = 0.5
TARGET_GAIN = 4.0
STEP = 4

SIM = ("z", "y", "xh")
LEARN = ("xl", "c")
RING = ("xh", "xl")
PLANE = ("z", "y")

BF16 = jnp.bfloat16
F32 = jnp.float32


def with_halo(x, sides, width):
    for axis, dim in sides:
        size, length = (lax.axis_size(axis), x.shape[dim])
        up = [(i, (i + 1) % size) for i in range(size)]
        down = [(j, i) for i, j in up]
        last = lax.slice_in_dim(x, length - width, length, axis=dim)
        first = lax.slice_in_dim(x, 0, width, axis=dim)
        before = lax.ppermute(last, axis, up)
        after = lax.ppermute(first, axis, down)
        x = jnp.concatenate([before, x, after], axis=dim)
    return x


def interior_step(padded, diffusion):
    center = padded[:, 1:-1, 1:-1]
    beside_all = padded[:, :-2, 1:-1] + padded[:, 2:, 1:-1]
    beside_all = beside_all + padded[:, 1:-1, :-2] + padded[:, 1:-1, 2:]
    return center + diffusion[:, None, None] * (beside_all - 4.0 * center)


def dot(a, b):
    return jnp.dot(a, b, preferred_element_type=F32)


def dot_t(a, b):
    return lax.dot_general(a, b, (((1,), (1,)), ((), ())), preferred_element_type=F32)


def activate(value):
    sigma = 0.5 * jnp.tanh(0.5 * value) + 0.5
    act = value * sigma
    return act.astype(BF16), sigma + act * (1.0 - sigma)


def network_kernel(
    count,
    meta,
    state,
    after,
    w1t,
    w2t,
    w2,
    w3t,
    w3,
    gin,
    gmid,
    gout,
    xbuf,
    abuf,
    slope1,
    slope2,
    sems,
):
    total = meta[0]
    steps = (total + STEP - 1) // STEP
    per_row = state.shape[2] // BW
    levels = w1t.shape[1]
    hid = w2.shape[0]

    def copies(step, slot, i):
        spot = meta[1 + step * STEP + i]
        row, col = spot // per_row, pl.multiple_of((spot % per_row) * BW, BW)
        lanes = pl.ds(i * BW, BW)
        return (
            pltpu.make_async_copy(
                state.at[:, row, pl.ds(col, BW)], xbuf.at[slot, :, lanes], sems.at[slot, i, 0]
            ),
            pltpu.make_async_copy(
                after.at[:, row, pl.ds(col, BW)], abuf.at[slot, :, lanes], sems.at[slot, i, 1]
            ),
        )

    def fetch(step, slot):
        for i in range(STEP):

            @pl.when(step * STEP + i < total)
            def _():
                for copy in copies(step, slot, i):
                    copy.start()

    gin[...] = jnp.zeros_like(gin)
    gmid[...] = jnp.zeros_like(gmid)
    gout[...] = jnp.zeros_like(gout)

    @pl.when(steps > 0)
    def _():
        fetch(0, 0)

    def body(step, carry):
        slot = lax.rem(step, 2)

        @pl.when(step + 1 < steps)
        def _():
            fetch(step + 1, 1 - slot)

        for i in range(STEP):
            index = step * STEP + i

            @pl.when(index < total)
            def _():
                for copy in copies(step, slot, i):
                    copy.wait()

            @pl.when(index >= total)
            def _():
                zero = jnp.zeros((levels, BW), F32)
                xbuf[slot, :, i * BW : (i + 1) * BW] = zero
                abuf[slot, :, i * BW : (i + 1) * BW] = zero

        x = xbuf[slot]
        inputs = x.astype(BF16)
        targets = (TARGET_GAIN * (abuf[slot] - x)).astype(BF16)
        act_one, slope1[...] = activate(dot(w1t[...], inputs))
        act_two, slope2[...] = activate(dot(w2t[...], act_one))
        output = dot(w3t[...], act_two)
        error = ((output - targets.astype(F32)) / count).astype(BF16)
        gout[...] += dot_t(act_two, error)
        delta_two = (dot(w3[...], error) * slope2[...]).astype(BF16)
        for j in range(0, hid, 2 * BW):
            both = dot_t(act_one, delta_two[j : j + 2 * BW])
            gmid[j // BW] += both[:, :BW]
            gmid[j // BW + 1] += both[:, BW:]
        delta_one = (dot(w2[...], delta_two) * slope1[...]).astype(BF16)
        for j in range(0, hid, 2 * BW):
            both = dot_t(inputs, delta_one[j : j + 2 * BW])
            gin[j // BW] += both[:, :BW]
            gin[j // BW + 1] += both[:, BW:]
        return carry

    lax.fori_loop(0, steps, body, 0)


def network(meta, state, after, weight_in, weight_mid, weight_out, count):
    levels, hid = weight_in.shape
    first, second, third = (w.astype(BF16) for w in (weight_in, weight_mid, weight_out))
    vmem = pl.BlockSpec(memory_space=pltpu.VMEM)
    hbm = pl.BlockSpec(memory_space=pl.ANY)
    width = STEP * BW
    return pl.pallas_call(
        functools.partial(network_kernel, count),
        out_shape=(
            jax.ShapeDtypeStruct((hid // BW, levels, BW), F32),
            jax.ShapeDtypeStruct((hid // BW, hid, BW), F32),
            jax.ShapeDtypeStruct((hid, levels), F32),
        ),
        in_specs=[pl.BlockSpec(memory_space=pltpu.SMEM), hbm, hbm] + [vmem] * 5,
        out_specs=(vmem, vmem, vmem),
        scratch_shapes=[
            pltpu.VMEM((2, levels, width), F32),
            pltpu.VMEM((2, levels, width), F32),
            pltpu.VMEM((hid, width), F32),
            pltpu.VMEM((hid, width), F32),
            pltpu.SemaphoreType.DMA((2, STEP, 2)),
        ],
        compiler_params=pltpu.CompilerParams(vmem_limit_bytes=56 * 1024 * 1024),
        name="network",
    )(meta, state, after, first.T, second.T, second, third.T, third)


def sum_everywhere(grad_in, grad_mid, grad_out):
    core = lax.axis_index("c")
    parts = [g.reshape(2, -1, BW) for g in (grad_in, grad_mid, grad_out)]
    other = [lax.dynamic_index_in_dim(g, 1 - core, 0, False) for g in parts]
    own = [lax.dynamic_index_in_dim(g, core, 0, False) for g in parts]

    def packed(g_in, g_mid, g_out):
        high = lax.reduce_precision(g_out, 8, 7)
        low = (g_out - high).astype(BF16)
        high = high.astype(BF16)
        return jnp.concatenate([g_in.astype(BF16), g_mid.astype(BF16), high, low])

    n_in, n_mid, n_out = (g.shape[0] for g in own)
    cut = (n_in, n_in + n_mid, n_in + n_mid + n_out)
    got = lax.ppermute(packed(*other), "c", [(0, 1), (1, 0)]).astype(F32)
    pair = packed(
        own[0] + got[: cut[0]],
        own[1] + got[cut[0] : cut[1]],
        own[2] + (got[cut[1] : cut[2]] + got[cut[2] :]),
    )
    ring, plane = lax.axis_size(RING), lax.axis_size(PLANE)
    held = lax.all_to_all(pair, RING, 0, 0, tiled=True)
    held = jnp.sum(held.reshape(ring, -1, BW).astype(F32), axis=0)
    held = lax.all_to_all(held, PLANE, 0, 0, tiled=True)
    held = jnp.sum(held.reshape(plane, -1, BW), axis=0)
    rows = held.shape[0]
    largest = jnp.max(jnp.abs(held))
    power = jnp.floor(jnp.log2(jnp.maximum(largest, 1e-30)))
    sent = (held * jnp.exp2(14.0 - power)).astype(jnp.float16)
    sent = jnp.concatenate([sent, jnp.full((8, BW), power, jnp.float16)])
    for axis, size in ((PLANE, plane), (RING, ring)):
        spread = jnp.broadcast_to(sent, (size,) + sent.shape).reshape(-1, BW)
        sent = lax.all_to_all(spread, axis, 0, 0, tiled=True)
    away = lax.ppermute(sent, "c", [(0, 1), (1, 0)])

    def opened(block):
        block = block.reshape(ring * plane, rows + 8, BW).astype(F32)
        scale = jnp.exp2(block[:, rows : rows + 1] - 14.0)
        return (block[:, :rows] * scale).reshape(-1, BW)

    mine, theirs = opened(sent), opened(away)
    low_half = jnp.where(core == 0, mine, theirs)
    high_half = jnp.where(core == 0, theirs, mine)
    halves = (low_half, high_half)
    total_in = jnp.concatenate([h[: cut[0]] for h in halves])
    total_mid = jnp.concatenate([h[cut[0] : cut[1]] for h in halves])
    total_out = jnp.concatenate([h[cut[1] : cut[2]] + h[cut[2] :] for h in halves])
    return total_in, total_mid, total_out


def on_device(state_field, diffusion, weight_in, weight_mid, weight_out, block_tile, block_pos):
    levels, tile_rows, tile_cols = state_field.shape
    padded = with_halo(state_field, ((SIM, 1), (LEARN, 2)), 2)
    after = interior_step(interior_step(padded, diffusion), diffusion)
    senders = lax.axis_size(SIM)
    own_index = lax.axis_index(SIM)
    samples = block_tile.shape[0] // senders
    tiles = block_tile[:, 0].reshape(senders, samples)
    places = block_pos.reshape(senders, samples)
    matched = tiles == own_index
    place = jnp.sum(jnp.where(matched, places, 0), axis=1)
    present = jnp.any(matched, axis=1)
    order = jnp.arange(senders)
    rank = jnp.sum(jnp.where(order[None, :] < order[:, None], present[None, :], False), axis=1)
    lands = present[:, None] & (rank[:, None] == order[None, :])
    slots = jnp.sum(jnp.where(lands, place[:, None], 0), axis=0)
    meta = jnp.concatenate([jnp.sum(present.astype(jnp.int32))[None], slots.astype(jnp.int32)])
    count = float(senders * lax.axis_size(LEARN) * samples * BW)
    grads = network(meta, state_field, after, weight_in, weight_mid, weight_out, count)
    total_in, total_mid, total_out = sum_everywhere(*grads)
    hid = weight_in.shape[1]
    total_in = jnp.swapaxes(total_in.reshape(hid // BW, levels, BW), 0, 1).reshape(levels, hid)
    total_mid = jnp.swapaxes(total_mid.reshape(hid // BW, hid, BW), 0, 1).reshape(hid, hid)
    new_in = weight_in - RATE * total_in
    new_mid = weight_mid - RATE * total_mid
    new_out = weight_out - RATE * total_out
    return (after, new_in, new_mid, new_out)


def solution(mesh):
    fine = Mesh(mesh.devices.reshape(4, 4, 2, 2, 2), SIM + LEARN)
    placed = (P(None, SIM, LEARN), P(), P(), P(), P(), P(LEARN, None), P(LEARN))
    return jax.shard_map(
        on_device,
        mesh=fine,
        in_specs=placed,
        out_specs=(P(None, SIM, LEARN), P(), P(), P()),
        check_vma=False,
    )
```

```python
import functools
import math

import jax
import jax.numpy as jnp
from jax import lax
from jax.experimental import pallas as pl
from jax.experimental.pallas import tpu as pltpu
from jax.sharding import Mesh
from jax.sharding import PartitionSpec as P

BW = 128
RATE = 0.5
TARGET_GAIN = 4.0
STEP = 4
SHARDS = 64

SIM = ("z", "y", "xh")
LEARN = ("xl", "c")
RING = ("xh", "xl")
PLANE = ("z", "y")

BF16 = jnp.bfloat16
F32 = jnp.float32


def shift(x, axis, by):
    size = lax.axis_size(axis)
    return lax.ppermute(x, axis, [(i, (i + by) % size) for i in range(size)])


def stencil_kernel(diffusion, state, edge_rows, edge_cols, corners, after, even, odd):
    chunk, rows, cols = state.shape
    base = pl.program_id(0) * chunk
    tall, wide = rows + 8, cols + BW

    def diffuse(field, at):
        rate = diffusion[base + at]
        beside = pltpu.roll(field, 1, 0) + pltpu.roll(field, tall - 1, 0)
        beside = beside + pltpu.roll(field, 1, 1) + pltpu.roll(field, wide - 1, 1)
        return (1.0 - 4.0 * rate) * field + rate * beside

    def first(at, held):
        upper = jnp.concatenate([state[at], edge_cols[at]], axis=1)
        lower = jnp.concatenate([edge_rows[at], corners[at]], axis=1)
        held[...] = diffuse(jnp.concatenate([upper, lower], axis=0), at)

    def second(at, held):
        after[at] = diffuse(held[...], at)[:rows, :cols]

    first(0, even)

    def pair(at, carry):
        first(2 * at + 1, odd)
        second(2 * at, even)
        first(jnp.minimum(2 * at + 2, chunk - 1), even)
        second(2 * at + 1, odd)
        return carry

    lax.fori_loop(0, chunk // 2, pair, 0, unroll=2)


def diffuse_twice(state, diffusion, later):
    levels, rows, cols = state.shape
    half = jnp.float16
    left = shift(jnp.transpose(state[:, :, cols - 2 :], (2, 1, 0)), LEARN, 1)
    right = shift(jnp.transpose(state[:, :, :2], (2, 1, 0)), LEARN, -1)

    def outgoing(first, at):
        ends = jnp.concatenate([left[1, at], right[0, at], jnp.zeros((cols - 2 * levels,), F32)])
        ends = jnp.stack([ends, jnp.zeros_like(ends)])[None]
        return jnp.concatenate([state[:, first : first + 2], ends]).astype(half)

    ends = (outgoing(rows - 2, rows - 1), outgoing(0, 0))
    ends, later = lax.optimization_barrier((ends, later))
    above = shift(ends[0], SIM, 1)
    below = shift(ends[1], SIM, -1)
    edge_cols = jnp.concatenate([right, jnp.zeros((BW - 4, rows, levels), F32), left])
    edge_cols = jnp.transpose(edge_cols, (2, 1, 0))
    gap = jnp.zeros((levels, 4, cols), F32)
    edge_rows = jnp.concatenate(
        [below[:levels].astype(F32), gap, above[:levels].astype(F32)], axis=1
    )
    row = lax.broadcasted_iota(jnp.int32, (levels, 8, BW), 1)
    lane = lax.broadcasted_iota(jnp.int32, (levels, 8, BW), 2)
    corners = jnp.zeros((levels, 8, BW), F32)
    for at, block in ((0, below), (7, above)):
        ends = block[levels, 0].astype(F32)
        for spot, value in ((BW - 1, ends[:levels]), (0, ends[levels : 2 * levels])):
            corners = jnp.where((row == at) & (lane == spot), value[:, None, None], corners)
    return stencil_call(state, edge_rows, edge_cols, corners, diffusion), later


def stencil_call(state, edge_rows, edge_cols, corners, diffusion):
    levels, rows, cols = state.shape
    chunk = 16

    def block(*shape):
        return pl.BlockSpec((chunk,) + shape, lambda i: (i, 0, 0))

    return pl.pallas_call(
        stencil_kernel,
        out_shape=jax.ShapeDtypeStruct(state.shape, F32),
        grid=(levels // chunk,),
        in_specs=[
            pl.BlockSpec(memory_space=pltpu.SMEM),
            block(rows, cols),
            block(8, cols),
            block(rows, BW),
            block(8, BW),
        ],
        out_specs=block(rows, cols),
        scratch_shapes=[pltpu.VMEM((rows + 8, cols + BW), F32)] * 2,
        name="stencil",
    )(diffusion, state, edge_rows, edge_cols, corners)


def dot(a, b):
    return jnp.dot(a, b, preferred_element_type=F32)


def dot_t(a, b):
    return lax.dot_general(a, b, (((1,), (1,)), ((), ())), preferred_element_type=F32)


def activate(value):
    sigma = 0.5 * jnp.tanh(0.5 * value) + 0.5
    act = value * sigma
    return act.astype(BF16), sigma + act * (1.0 - sigma)


def store_split(target, block):
    high = block.astype(BF16)
    low = (block[:, 72:] - high[:, 72:].astype(F32)).astype(BF16)
    target[:, :80], target[:, 80:] = high, low


def network_kernel(
    count, meta, state, after, w1t, w2t, w2, w3t, w3, grads, send, xbuf, abuf, slope1, slope2, sems
):
    total, core = meta[0], meta[1]
    steps = (total + STEP - 1) // STEP
    per_row = state.shape[2] // BW
    levels = w1t.shape[1]
    hid = w2.shape[0]

    def copies(step, slot, i):
        spot = meta[2 + step * STEP + i]
        row, col = spot // per_row, pl.multiple_of((spot % per_row) * BW, BW)
        lanes = pl.ds(i * BW, BW)
        return (
            pltpu.make_async_copy(
                state.at[:, row, pl.ds(col, BW)], xbuf.at[slot, :, lanes], sems.at[slot, i, 0]
            ),
            pltpu.make_async_copy(
                after.at[:, row, pl.ds(col, BW)], abuf.at[slot, :, lanes], sems.at[slot, i, 1]
            ),
        )

    def fetch(step, slot):
        for i in range(STEP):

            @pl.when(step * STEP + i < total)
            def _():
                for copy in copies(step, slot, i):
                    copy.start()

    @pl.when(steps > 0)
    def _():
        fetch(0, 0)

    grads[...] = jnp.zeros_like(grads)

    def body(step, carry):
        slot = lax.rem(step, 2)

        @pl.when(step + 1 < steps)
        def _():
            fetch(step + 1, 1 - slot)

        for i in range(STEP):
            index = step * STEP + i

            @pl.when(index < total)
            def _():
                for copy in copies(step, slot, i):
                    copy.wait()

            @pl.when(index >= total)
            def _():
                zero = jnp.zeros((levels, BW), F32)
                xbuf[slot, :, i * BW : (i + 1) * BW] = zero
                abuf[slot, :, i * BW : (i + 1) * BW] = zero

        x = xbuf[slot]
        inputs = x.astype(BF16)
        targets = (TARGET_GAIN * (abuf[slot] - x)).astype(BF16)
        act_one, slope1[...] = activate(dot(w1t[...], inputs))
        act_two, slope2[...] = activate(dot(w2t[...], act_one))
        output = dot(w3t[...], act_two)
        error = ((output - targets.astype(F32)) / count).astype(BF16)
        grads[:, :, :, 72:] += dot_t(act_two, error).reshape(2, 8, 8, 8, BW)
        delta_two = (dot(w3[...], error) * slope2[...]).astype(BF16)
        for j in range(0, hid // BW, 2):
            both = dot_t(act_one, delta_two[j * BW : (j + 2) * BW])
            for k in (0, 1):
                at = (j + k) * 8
                grads[:, :, :, at : at + 8] += both[:, k * BW : (k + 1) * BW].reshape(2, 8, 8, 8, BW)
        delta_one = (dot(w2[...], delta_two) * slope1[...]).astype(BF16)
        for j in range(0, hid // BW, 2):
            both = dot_t(inputs, delta_one[j * BW : (j + 2) * BW])
            for k in (0, 1):
                grads[:, :, j + k, 64:72] += both[:, k * BW : (k + 1) * BW].reshape(2, 8, 8, BW)
        return carry

    lax.fori_loop(0, steps, body, 0)
    store_split(send, grads[1 - core].reshape(SHARDS, 80, BW))


def network(meta, state, after, weight_in, weight_mid, weight_out, count):
    levels, hid = weight_in.shape
    first, second, third = (w.astype(BF16) for w in (weight_in, weight_mid, weight_out))
    vmem = pl.BlockSpec(memory_space=pltpu.VMEM)
    hbm = pl.BlockSpec(memory_space=pl.ANY)
    width = STEP * BW
    return pl.pallas_call(
        functools.partial(network_kernel, count),
        out_shape=(
            jax.ShapeDtypeStruct((2, 8, 8, 80, BW), F32),
            jax.ShapeDtypeStruct((SHARDS, 88, BW), BF16),
        ),
        in_specs=[pl.BlockSpec(memory_space=pltpu.SMEM), hbm, hbm] + [vmem] * 5,
        out_specs=(vmem, vmem),
        scratch_shapes=[
            pltpu.VMEM((2, levels, width), F32),
            pltpu.VMEM((2, levels, width), F32),
            pltpu.VMEM((hid, width), F32),
            pltpu.VMEM((hid, width), F32),
            pltpu.SemaphoreType.DMA((2, STEP, 2)),
        ],
        compiler_params=pltpu.CompilerParams(vmem_limit_bytes=56 * 1024 * 1024),
        name="network",
    )(meta, state, after, first.T, second.T, second, third.T, third)


def update_kernel(half, total, w_in, w_mid, w_out, *rest):
    new_in, new_mid, new_out = rest[-3:]
    for a in range(total.shape[0]):
        for b in range(8):
            step = RATE * total[a, b]
            lanes = slice(b * BW, (b + 1) * BW)
            rows = slice(a * 8, (a + 1) * 8)
            new_in[rows, lanes] = w_in[rows, lanes] - step[64:72]
            rows = slice(a * 64 + b * 8, a * 64 + (b + 1) * 8)
            new_out[rows, :] = w_out[rows, :] - step[72:]
            for j in range(8):
                lanes = slice(j * BW, (j + 1) * BW)
                new_mid[rows, lanes] = w_mid[rows, lanes] - step[j * 8 : (j + 1) * 8]


def update(half, total, weights, news):
    hid = weights[1].shape[0]
    a = 2
    steps = 8 // a
    blocks = [
        pl.BlockSpec((8 * a, hid), lambda i, half: (half[0] * steps + i, 0)),
        pl.BlockSpec((64 * a, hid), lambda i, half: (half[0] * steps + i, 0)),
        pl.BlockSpec((64 * a, BW), lambda i, half: (half[0] * steps + i, 0)),
    ]
    kept = [pl.BlockSpec(memory_space=pl.ANY)] * len(news)
    return pl.pallas_call(
        update_kernel,
        out_shape=[jax.ShapeDtypeStruct(w.shape, F32) for w in weights],
        grid_spec=pltpu.PrefetchScalarGridSpec(
            num_scalar_prefetch=1,
            grid=(steps,),
            in_specs=[pl.BlockSpec((a, 8, 80, BW), lambda i, half: (i, 0, 0, 0))] + blocks + kept,
            out_specs=blocks,
        ),
        input_output_aliases={5 + i: i for i in range(len(news))},
        cost_estimate=pl.CostEstimate(flops=20_000_000, bytes_accessed=8_000_000, transcendentals=0),
        name="update",
    )(half[None], total, *weights, *news)


def sum_everywhere(grads, send, weights):
    core = lax.axis_index("c")
    swap = [(0, 1), (1, 0)]
    got = lax.ppermute(send, "c", swap).astype(F32)
    pair = lax.dynamic_index_in_dim(grads, core, 0, False).reshape(SHARDS, 80, BW)
    pair = pair + got[:, :80]
    last = pair[:, 72:] + got[:, 80:]
    high = lax.reduce_precision(last, 8, 7)
    pair = jnp.concatenate([pair[:, :72], high, last - high], axis=1).astype(BF16)
    ring, plane = lax.axis_size(RING), lax.axis_size(PLANE)
    held = lax.all_to_all(pair.reshape(-1, BW), PLANE, 0, 0, tiled=True)
    held = jnp.sum(held.reshape(plane, -1, BW).astype(F32), axis=0)
    held = lax.all_to_all(held, RING, 0, 0, tiled=True)
    held = jnp.sum(held.reshape(ring, -1, BW), axis=0)
    held = jnp.concatenate([held[:72], held[72:80] + held[80:]])
    power = jnp.floor(jnp.log2(jnp.maximum(jnp.max(jnp.abs(held)), 1e-30)))
    sent = (held * jnp.exp2(14.0 - power)).astype(jnp.float16)
    sent = jnp.concatenate([sent, jnp.full((8, BW), power, jnp.float16)])
    for axis, size in ((RING, ring), (PLANE, plane)):
        spread = jnp.broadcast_to(sent, (size,) + sent.shape).reshape(-1, BW)
        sent = lax.all_to_all(spread, axis, 0, 0, tiled=True)
    away = lax.ppermute(sent, "c", swap)

    def opened(block):
        block = block.reshape(SHARDS, 88, BW).astype(F32)
        return (block[:, :80] * jnp.exp2(block[:, 80:81] - 14.0)).reshape(8, 8, 80, BW)

    news = update(core, opened(sent), weights, ())
    return update(1 - core, opened(away), weights, news)


def on_device(state_field, diffusion, weight_in, weight_mid, weight_out, block_tile, block_pos):
    levels, tile_rows, tile_cols = state_field.shape
    weights = (weight_in, weight_mid, weight_out)
    after, late = diffuse_twice(state_field, diffusion, (weights, block_tile, block_pos))
    late_weights, block_tile, block_pos = late
    senders = lax.axis_size(SIM)
    own_index = lax.axis_index(SIM)
    samples = block_tile.shape[0] // senders
    tiles = block_tile[:, 0].reshape(senders, samples)
    places = block_pos.reshape(senders, samples)
    matched = tiles == own_index
    place = jnp.sum(jnp.where(matched, places, 0), axis=1)
    present = jnp.any(matched, axis=1)
    order = jnp.arange(senders)
    rank = jnp.sum(jnp.where(order[None, :] < order[:, None], present[None, :], False), axis=1)
    lands = present[:, None] & (rank[:, None] == order[None, :])
    slots = jnp.sum(jnp.where(lands, place[:, None], 0), axis=0)
    total = jnp.sum(present.astype(jnp.int32))
    meta = jnp.concatenate([jnp.stack([total, lax.axis_index("c")]), slots.astype(jnp.int32)])
    count = float(senders * lax.axis_size(LEARN) * samples * BW)
    grads, send = network(meta, state_field, after, *late_weights, count)
    new_in, new_mid, new_out = sum_everywhere(grads, send, weights)
    return (after, new_in, new_mid, new_out)


def solution(mesh):
    fine = Mesh(mesh.devices.reshape(4, 4, 2, 2, 2), SIM + LEARN)
    placed = (P(None, SIM, LEARN), P(), P(), P(), P(), P(LEARN, None), P(LEARN))
    return jax.shard_map(
        on_device,
        mesh=fine,
        in_specs=placed,
        out_specs=(P(None, SIM, LEARN), P(), P(), P()),
        check_vma=False,
    )
```

```python
import functools

import jax
import jax.numpy as jnp
from jax import lax
from jax.experimental import pallas as pl
from jax.experimental.pallas import tpu as pltpu
from jax.sharding import Mesh
from jax.sharding import PartitionSpec as P


BW = 128
RATE = 0.5
TARGET_GAIN = 4.0
STEP = 4
SHARDS = 64

SIM = ("z", "y", "xh")
LEARN = ("xl", "c")
RING = ("xh", "xl")
PLANE = ("z", "y")

BF16 = jnp.bfloat16
F32 = jnp.float32


def shift(x, axis, by):
    size = lax.axis_size(axis)
    return lax.ppermute(x, axis, [(i, (i + by) % size) for i in range(size)])


GROUP = 8


def stencil_kernel(diffusion, state, edge_rows, edge_cols, corners, after, *held):
    chunk, rows, cols = state.shape
    base = pl.program_id(0) * chunk
    tall, wide = rows + 8, cols + BW
    fields, beside = held

    def sideways(field):
        return pltpu.roll(field, 1, 1) + pltpu.roll(field, wide - 1, 1)

    def diffuse(g, at):
        rate = diffusion[base + at]
        field = fields[g]
        around = pltpu.roll(field, 1, 0) + pltpu.roll(field, tall - 1, 0) + beside[g]
        return (1.0 - 4.0 * rate) * field + rate * around

    def group(index, carry):
        spots = [(g, index * GROUP + g) for g in range(GROUP)]
        for g, at in spots:
            upper = jnp.concatenate([state[at], edge_cols[at]], axis=1)
            lower = jnp.concatenate([edge_rows[at], corners[at]], axis=1)
            field = jnp.concatenate([upper, lower], axis=0)
            fields[g] = field
            beside[g] = sideways(field)
        for g, at in spots:
            fields[g] = diffuse(g, at)
        for g, at in spots:
            beside[g] = sideways(fields[g])
        for g, at in spots:
            after[at] = diffuse(g, at)[:rows, :cols]
        return carry

    lax.fori_loop(0, chunk // GROUP, group, 0)


def exchange(state, later):
    levels, rows, cols = state.shape
    half = jnp.float16
    left = shift(jnp.transpose(state[:, :, cols - 2 :], (2, 1, 0)), LEARN, 1)
    right = shift(jnp.transpose(state[:, :, :2], (2, 1, 0)), LEARN, -1)

    def outgoing(first, at):
        ends = jnp.concatenate([left[1, at], right[0, at], jnp.zeros((cols - 2 * levels,), F32)])
        ends = jnp.stack([ends, jnp.zeros_like(ends)])[None]
        return jnp.concatenate([state[:, first : first + 2], ends]).astype(half)

    ends = (outgoing(rows - 2, rows - 1), outgoing(0, 0))
    ends, later = lax.optimization_barrier((ends, later))
    above = shift(ends[0], SIM, 1)
    below = shift(ends[1], SIM, -1)

    def edges():
        edge_cols = jnp.concatenate([right, jnp.zeros((BW - 4, rows, levels), F32), left])
        edge_cols = jnp.transpose(edge_cols, (2, 1, 0))
        gap = jnp.zeros((levels, 4, cols), F32)
        edge_rows = jnp.concatenate(
            [below[:levels].astype(F32), gap, above[:levels].astype(F32)], axis=1
        )
        row = lax.broadcasted_iota(jnp.int32, (levels, 8, BW), 1)
        lane = lax.broadcasted_iota(jnp.int32, (levels, 8, BW), 2)
        corners = jnp.zeros((levels, 8, BW), F32)
        for at, block in ((0, below), (7, above)):
            tips = block[levels, 0].astype(F32)
            for spot, value in ((BW - 1, tips[:levels]), (0, tips[levels : 2 * levels])):
                corners = jnp.where((row == at) & (lane == spot), value[:, None, None], corners)
        return edge_rows, edge_cols, corners

    return edges, later


def stencil_call(state, edge_rows, edge_cols, corners, diffusion):
    levels, rows, cols = state.shape
    chunk = 32

    def block(*shape):
        return pl.BlockSpec((chunk,) + shape, lambda i: (i, 0, 0))

    return pl.pallas_call(
        stencil_kernel,
        out_shape=jax.ShapeDtypeStruct(state.shape, F32),
        grid=(levels // chunk,),
        in_specs=[
            pl.BlockSpec(memory_space=pltpu.SMEM),
            block(rows, cols),
            block(8, cols),
            block(rows, BW),
            block(8, BW),
        ],
        out_specs=block(rows, cols),
        scratch_shapes=[pltpu.VMEM((GROUP, rows + 8, cols + BW), F32)] * 2,
        name="stencil",
    )(diffusion, state, edge_rows, edge_cols, corners)


def dot(a, b):
    return jnp.dot(a, b, preferred_element_type=F32)


def dot_t(a, b):
    return lax.dot_general(a, b, (((1,), (1,)), ((), ())), preferred_element_type=F32)


def activate(value):
    sigma = 0.5 * jnp.tanh(0.5 * value) + 0.5
    act = value * sigma
    return act.astype(BF16), sigma + act * (1.0 - sigma)


def store_split(target, block):
    high = block.astype(BF16)
    low = (block[:, 72:] - high[:, 72:].astype(F32)).astype(BF16)
    target[:, :80], target[:, 80:] = high, low


def prepare_kernel(where, tiles, places, w_in, w_mid, w_out, meta, w1t, w2t, w2, w3t, w3, held):
    w1t[...] = w_in[...].T.astype(BF16)
    w2t[...] = w_mid[...].T.astype(BF16)
    w2[...] = w_mid[...].astype(BF16)
    w3t[...] = w_out[...].T.astype(BF16)
    w3[...] = w_out[...].astype(BF16)
    groups = (meta.shape[0] - 2) // 2
    samples = tiles.shape[0] // groups

    def clear(i, carry):
        held[i] = 0
        return carry

    lax.fori_loop(0, held.shape[0], clear, 0)

    def group(g, count):
        place = -1
        for k in range(samples):
            place = jnp.where(tiles[g * samples + k] == where[0], places[g * samples + k], place)
        spot = jnp.maximum(place, 0)
        earlier = held[spot]
        fresh = (place >= 0) & (earlier == 0)

        @pl.when((place >= 0) & (earlier > 0))
        def _():
            meta[2 + groups + earlier - 1] = 2
            held[spot] = 0

        @pl.when(fresh)
        def _():
            meta[2 + count] = spot
            meta[2 + groups + count] = 1
            held[spot] = count + 1

        return count + fresh.astype(jnp.int32)

    meta[0] = lax.fori_loop(0, groups, group, 0)
    meta[1] = where[1]


def prepare(where, tiles, places, weights, groups, spots):
    levels, hid = weights[0].shape
    smem = pl.BlockSpec(memory_space=pltpu.SMEM)
    vmem = pl.BlockSpec(memory_space=pltpu.VMEM)
    shapes = ((hid, levels), (hid, hid), (hid, hid), (levels, hid), (hid, levels))
    return pl.pallas_call(
        prepare_kernel,
        out_shape=[jax.ShapeDtypeStruct((2 + 2 * groups,), jnp.int32)]
        + [jax.ShapeDtypeStruct(shape, BF16) for shape in shapes],
        in_specs=[smem] * 3 + [vmem] * 3,
        out_specs=[smem] + [vmem] * 5,
        scratch_shapes=[pltpu.SMEM((spots,), jnp.int32)],
        cost_estimate=pl.CostEstimate(flops=20_000_000, bytes_accessed=9_000_000, transcendentals=0),
        name="prepare",
    )(where, tiles, places, *weights)


def network_kernel(count, meta, state, after, *refs):
    given, (own, send, grads), kept = refs[:5], refs[5:8], refs[8:13]
    xbuf, abuf, slope1, slope2, sems, loads, leave = refs[13:]
    w1t, w2t, w2, w3t, w3 = kept
    total, core = meta[0], meta[1]
    steps = (total + STEP - 1) // STEP
    per_row = state.shape[2] // BW
    levels = w1t.shape[1]
    hid = w2.shape[0]
    groups = (meta.shape[0] - 2) // 2

    def copies(step, slot, i):
        spot = meta[2 + step * STEP + i]
        row, col = spot // per_row, pl.multiple_of((spot % per_row) * BW, BW)
        lanes = pl.ds(i * BW, BW)
        return (
            pltpu.make_async_copy(
                state.at[:, row, pl.ds(col, BW)], xbuf.at[slot, :, lanes], sems.at[slot, i, 0]
            ),
            pltpu.make_async_copy(
                after.at[:, row, pl.ds(col, BW)], abuf.at[slot, :, lanes], sems.at[slot, i, 1]
            ),
        )

    def fetch(step, slot):
        for i in range(STEP):

            @pl.when(step * STEP + i < total)
            def _():
                for copy in copies(step, slot, i):
                    copy.start()

    @pl.when(steps > 0)
    def _():
        fetch(0, 0)

    moves = [pltpu.make_async_copy(given[i], kept[i], loads.at[i]) for i in range(5)]
    for move in moves:
        move.start()
    grads[...] = jnp.zeros_like(grads)
    lane = lax.broadcasted_iota(jnp.int32, (1, STEP * BW), 1) // BW
    for move in moves:
        move.wait()

    def body(step, carry):
        slot = lax.rem(step, 2)

        @pl.when(step + 1 < steps)
        def _():
            fetch(step + 1, 1 - slot)

        for i in range(STEP):
            index = step * STEP + i

            @pl.when(index < total)
            def _():
                for copy in copies(step, slot, i):
                    copy.wait()

            @pl.when(index >= total)
            def _():
                zero = jnp.zeros((levels, BW), F32)
                xbuf[slot, :, i * BW : (i + 1) * BW] = zero
                abuf[slot, :, i * BW : (i + 1) * BW] = zero

        x = xbuf[slot]
        inputs = x.astype(BF16)
        targets = (TARGET_GAIN * (abuf[slot] - x)).astype(BF16)
        act_one, slope1[...] = activate(dot(w1t[...], inputs))
        act_two, slope2[...] = activate(dot(w2t[...], act_one))
        output = dot(w3t[...], act_two)
        times = jnp.ones((1, STEP * BW), F32)
        for i in range(STEP):
            index = step * STEP + i
            often = jnp.where(index < total, meta[2 + groups + jnp.minimum(index, groups - 1)], 1)
            times = jnp.where(lane == i, often.astype(F32), times)
        error = ((output - targets.astype(F32)) / count).astype(BF16)
        error = (error.astype(F32) * times).astype(BF16)
        grads[:, :, :, 72:] += dot_t(act_two, error).reshape(2, 8, 8, 8, BW)
        delta_two = (dot(w3[...], error) * slope2[...]).astype(BF16)
        for j in range(0, hid // BW, 2):
            both = dot_t(act_one, delta_two[j * BW : (j + 2) * BW])
            for k in (0, 1):
                at = (j + k) * 8
                grads[:, :, :, at : at + 8] += both[:, k * BW : (k + 1) * BW].reshape(2, 8, 8, 8, BW)
        delta_one = (dot(w2[...], delta_two) * slope1[...]).astype(BF16)
        for j in range(0, hid // BW, 2):
            both = dot_t(inputs, delta_one[j * BW : (j + 2) * BW])
            for k in (0, 1):
                grads[:, :, j + k, 64:72] += both[:, k * BW : (k + 1) * BW].reshape(2, 8, 8, BW)
        return carry

    lax.fori_loop(0, steps, body, 0)
    out = pltpu.make_async_copy(grads.at[core], own, leave)
    out.start()
    store_split(send, grads[1 - core].reshape(SHARDS, 80, BW))
    out.wait()


def network(meta, state, after, ready, count):
    hid, levels = ready[0].shape
    vmem = pl.BlockSpec(memory_space=pltpu.VMEM)
    hbm = pl.BlockSpec(memory_space=pl.ANY)
    width = STEP * BW
    return pl.pallas_call(
        functools.partial(network_kernel, count),
        out_shape=(
            jax.ShapeDtypeStruct((8, 8, 80, BW), F32),
            jax.ShapeDtypeStruct((SHARDS, 88, BW), BF16),
        ),
        in_specs=[pl.BlockSpec(memory_space=pltpu.SMEM)] + [hbm] * 7,
        out_specs=(hbm, vmem),
        scratch_shapes=[pltpu.VMEM((2, 8, 8, 80, BW), F32)]
        + [pltpu.VMEM(w.shape, BF16) for w in ready]
        + [
            pltpu.VMEM((2, levels, width), F32),
            pltpu.VMEM((2, levels, width), F32),
            pltpu.VMEM((hid, width), F32),
            pltpu.VMEM((hid, width), F32),
            pltpu.SemaphoreType.DMA((2, STEP, 2)),
            pltpu.SemaphoreType.DMA((5,)),
            pltpu.SemaphoreType.DMA,
        ],
        compiler_params=pltpu.CompilerParams(vmem_limit_bytes=56 * 1024 * 1024),
        name="network",
    )(meta, state, after, *ready)


def update_kernel(half, total, w_in, w_mid, w_out, *rest):
    new_in, new_mid, new_out = rest[-3:]
    for a in range(total.shape[0]):
        for b in range(8):
            step = RATE * total[a, b]
            lanes = slice(b * BW, (b + 1) * BW)
            rows = slice(a * 8, (a + 1) * 8)
            new_in[rows, lanes] = w_in[rows, lanes] - step[64:72]
            rows = slice(a * 64 + b * 8, a * 64 + (b + 1) * 8)
            new_out[rows, :] = w_out[rows, :] - step[72:]
            for j in range(8):
                lanes = slice(j * BW, (j + 1) * BW)
                new_mid[rows, lanes] = w_mid[rows, lanes] - step[j * 8 : (j + 1) * 8]


def update(half, total, weights, news):
    hid = weights[1].shape[0]
    a = 2
    steps = 8 // a
    blocks = [
        pl.BlockSpec((8 * a, hid), lambda i, half: (half[0] * steps + i, 0)),
        pl.BlockSpec((64 * a, hid), lambda i, half: (half[0] * steps + i, 0)),
        pl.BlockSpec((64 * a, BW), lambda i, half: (half[0] * steps + i, 0)),
    ]
    kept = [pl.BlockSpec(memory_space=pl.ANY)] * len(news)
    return pl.pallas_call(
        update_kernel,
        out_shape=[jax.ShapeDtypeStruct(w.shape, F32) for w in weights],
        grid_spec=pltpu.PrefetchScalarGridSpec(
            num_scalar_prefetch=1,
            grid=(steps,),
            in_specs=[pl.BlockSpec((a, 8, 80, BW), lambda i, half: (i, 0, 0, 0))] + blocks + kept,
            out_specs=blocks,
        ),
        input_output_aliases={5 + i: i for i in range(len(news))},
        cost_estimate=pl.CostEstimate(flops=20_000_000, bytes_accessed=8_000_000, transcendentals=0),
        name="update",
    )(half[None], total, *weights, *news)


def sum_everywhere(own, send, weights):
    core = lax.axis_index("c")
    swap = [(0, 1), (1, 0)]
    got = lax.ppermute(send, "c", swap).astype(F32)
    pair = own.reshape(SHARDS, 80, BW) + got[:, :80]
    last = pair[:, 72:] + got[:, 80:]
    high = lax.reduce_precision(last, 8, 7)
    pair = jnp.concatenate([pair[:, :72], high, last - high], axis=1).astype(BF16)
    ring, plane = lax.axis_size(RING), lax.axis_size(PLANE)
    held = lax.all_to_all(pair.reshape(-1, BW), PLANE, 0, 0, tiled=True)
    held = jnp.sum(held.reshape(plane, -1, BW).astype(F32), axis=0)
    held = lax.all_to_all(held, RING, 0, 0, tiled=True)
    held = jnp.sum(held.reshape(ring, -1, BW), axis=0)
    held = jnp.concatenate([held[:72], held[72:80] + held[80:]])
    power = jnp.floor(jnp.log2(jnp.maximum(jnp.max(jnp.abs(held)), 1e-30)))
    sent = (held * jnp.exp2(14.0 - power)).astype(jnp.float16)
    sent = jnp.concatenate([sent, jnp.full((8, BW), power, jnp.float16)])
    for axis, size in ((RING, ring), (PLANE, plane)):
        spread = jnp.broadcast_to(sent, (size,) + sent.shape).reshape(-1, BW)
        sent = lax.all_to_all(spread, axis, 0, 0, tiled=True)
    away = lax.ppermute(sent, "c", swap)

    def opened(block):
        block = block.reshape(SHARDS, 88, BW).astype(F32)
        return (block[:, :80] * jnp.exp2(block[:, 80:81] - 14.0)).reshape(8, 8, 80, BW)

    news = update(core, opened(sent), weights, ())
    return update(1 - core, opened(away), weights, news)


def on_device(state_field, diffusion, weight_in, weight_mid, weight_out, block_tile, block_pos):
    senders = lax.axis_size(SIM)
    samples = block_tile.shape[0] // senders
    _, tile_rows, tile_cols = state_field.shape
    weights = (weight_in, weight_mid, weight_out)
    where = jnp.stack([lax.axis_index(SIM), lax.axis_index("c")]).astype(jnp.int32)
    edges, late = exchange(state_field, (where, block_tile[:, 0], block_pos))
    meta, *ready = prepare(*late, weights, senders, tile_rows * tile_cols // BW)
    after = stencil_call(state_field, *edges(), diffusion)
    count = float(senders * lax.axis_size(LEARN) * samples * BW)
    own, send = network(meta, state_field, after, ready, count)
    new_in, new_mid, new_out = sum_everywhere(own, send, weights)
    return (after, new_in, new_mid, new_out)


def solution(mesh):
    fine = Mesh(mesh.devices.reshape(4, 4, 2, 2, 2), SIM + LEARN)
    placed = (P(None, SIM, LEARN), P(), P(), P(), P(), P(LEARN, None), P(LEARN))
    return jax.shard_map(
        on_device,
        mesh=fine,
        in_specs=placed,
        out_specs=(P(None, SIM, LEARN), P(), P(), P()),
        check_vma=False,
    )
```

```python
import functools

import jax
import jax.numpy as jnp
from jax import lax
from jax.experimental import pallas as pl
from jax.experimental.pallas import tpu as pltpu
from jax.sharding import Mesh
from jax.sharding import PartitionSpec as P


BW = 128
RATE = 0.5
TARGET_GAIN = 4.0
STEP = 4
SHARDS = 64

SIM = ("z", "y", "xh")
LEARN = ("xl", "c")
RING = ("xh", "xl")
PLANE = ("z", "y")

BF16 = jnp.bfloat16
F32 = jnp.float32


def shift(x, axis, by):
    size = lax.axis_size(axis)
    return lax.ppermute(x, axis, [(i, (i + by) % size) for i in range(size)])


GROUP = 8


def stencil_kernel(diffusion, tips, state, below, above, edge_cols, after, *held):
    chunk, rows, cols = state.shape
    base = pl.program_id(0) * chunk
    tall, wide = rows + 8, cols + BW
    fields, beside = held
    row = lax.broadcasted_iota(jnp.int32, (8, BW), 0)
    lane = lax.broadcasted_iota(jnp.int32, (8, BW), 1)
    gap = jnp.zeros((4, cols), F32)
    ends = [(at, spot) for at in (0, 7) for spot in (BW - 1, 0)]

    def sideways(field):
        return pltpu.roll(field, 1, 1) + pltpu.roll(field, wide - 1, 1)

    def diffuse(g, at):
        rate = diffusion[base + at]
        field = fields[g]
        around = pltpu.roll(field, 1, 0) + pltpu.roll(field, tall - 1, 0) + beside[g]
        return (1.0 - 4.0 * rate) * field + rate * around

    def group(index, carry):
        spots = [(g, index * GROUP + g) for g in range(GROUP)]
        for g, at in spots:
            upper = jnp.concatenate([state[at], edge_cols[at]], axis=1)
            corners = jnp.zeros((8, BW), F32)
            for tip, (end, spot) in enumerate(ends):
                corners = jnp.where((row == end) & (lane == spot), tips[tip, base + at], corners)
            lower = jnp.concatenate([below[at], gap, above[at]], axis=0)
            lower = jnp.concatenate([lower, corners], axis=1)
            field = jnp.concatenate([upper, lower], axis=0)
            fields[g] = field
            beside[g] = sideways(field)
        for g, at in spots:
            fields[g] = diffuse(g, at)
        for g, at in spots:
            beside[g] = sideways(fields[g])
        for g, at in spots:
            after[at] = diffuse(g, at)[:rows, :cols]
        return carry

    lax.fori_loop(0, chunk // GROUP, group, 0)


def exchange(state, later):
    levels, rows, cols = state.shape
    half = jnp.float16
    left = shift(jnp.transpose(state[:, :, cols - 2 :], (2, 1, 0)), LEARN, 1)
    right = shift(jnp.transpose(state[:, :, :2], (2, 1, 0)), LEARN, -1)

    def outgoing(first, at):
        ends = jnp.concatenate([left[1, at], right[0, at], jnp.zeros((cols - 2 * levels,), F32)])
        ends = jnp.stack([ends, jnp.zeros_like(ends)])[None]
        return jnp.concatenate([state[:, first : first + 2], ends]).astype(half)

    ends = (outgoing(rows - 2, rows - 1), outgoing(0, 0))
    ends, later = lax.optimization_barrier((ends, later))
    above = shift(ends[0], SIM, 1)
    below = shift(ends[1], SIM, -1)

    def edges():
        edge_cols = jnp.concatenate([right, jnp.zeros((BW - 4, rows, levels), F32), left])
        edge_cols = jnp.transpose(edge_cols, (2, 1, 0))
        below_f32, above_f32 = below.astype(F32), above.astype(F32)
        tips = jnp.concatenate(
            [block[levels, 0, : 2 * levels].reshape(2, levels) for block in (below_f32, above_f32)]
        )
        return tips, below_f32, above_f32, edge_cols

    return edges, later


def stencil_call(state, tips, below, above, edge_cols, diffusion):
    levels, rows, cols = state.shape
    chunk = 32

    def block(*shape):
        return pl.BlockSpec((chunk,) + shape, lambda i: (i, 0, 0))

    smem = pl.BlockSpec(memory_space=pltpu.SMEM)
    return pl.pallas_call(
        stencil_kernel,
        out_shape=jax.ShapeDtypeStruct(state.shape, F32),
        grid=(levels // chunk,),
        in_specs=[smem, smem, block(rows, cols)]
        + [block(2, cols), block(2, cols), block(rows, BW)],
        out_specs=block(rows, cols),
        scratch_shapes=[pltpu.VMEM((GROUP, rows + 8, cols + BW), F32)] * 2,
        name="stencil",
    )(diffusion, tips, state, below, above, edge_cols)


def dot(a, b):
    return jnp.dot(a, b, preferred_element_type=F32)


def dot_t(a, b):
    return lax.dot_general(a, b, (((1,), (1,)), ((), ())), preferred_element_type=F32)


def activate(value):
    sigma = 0.5 * jnp.tanh(0.5 * value) + 0.5
    act = value * sigma
    return act.astype(BF16), sigma + act * (1.0 - sigma)


def store_split(target, block):
    high = block.astype(BF16)
    low = (block[:, 72:] - high[:, 72:].astype(F32)).astype(BF16)
    target[:, :80], target[:, 80:] = high, low


def prepare_kernel(where, tiles, places, w_in, w_mid, w_out, meta, w1t, w2t, w2, w3t, w3, held):
    w1t[...] = w_in[...].T.astype(BF16)
    w2t[...] = w_mid[...].T.astype(BF16)
    w2[...] = w_mid[...].astype(BF16)
    w3t[...] = w_out[...].T.astype(BF16)
    w3[...] = w_out[...].astype(BF16)
    groups = (meta.shape[0] - 2) // 2
    samples = tiles.shape[0] // groups

    def clear(i, carry):
        held[i] = 0
        return carry

    lax.fori_loop(0, held.shape[0], clear, 0)

    def group(g, count):
        place = -1
        for k in range(samples):
            place = jnp.where(tiles[g * samples + k] == where[0], places[g * samples + k], place)
        spot = jnp.maximum(place, 0)
        earlier = held[spot]
        fresh = (place >= 0) & (earlier == 0)

        @pl.when((place >= 0) & (earlier > 0))
        def _():
            meta[2 + groups + earlier - 1] = 2
            held[spot] = 0

        @pl.when(fresh)
        def _():
            meta[2 + count] = spot
            meta[2 + groups + count] = 1
            held[spot] = count + 1

        return count + fresh.astype(jnp.int32)

    meta[0] = lax.fori_loop(0, groups, group, 0)
    meta[1] = where[1]


def prepare(where, tiles, places, weights, groups, spots):
    levels, hid = weights[0].shape
    smem = pl.BlockSpec(memory_space=pltpu.SMEM)
    vmem = pl.BlockSpec(memory_space=pltpu.VMEM)
    shapes = ((hid, levels), (hid, hid), (hid, hid), (levels, hid), (hid, levels))
    return pl.pallas_call(
        prepare_kernel,
        out_shape=[jax.ShapeDtypeStruct((2 + 2 * groups,), jnp.int32)]
        + [jax.ShapeDtypeStruct(shape, BF16) for shape in shapes],
        in_specs=[smem] * 3 + [vmem] * 3,
        out_specs=[smem] + [vmem] * 5,
        scratch_shapes=[pltpu.SMEM((spots,), jnp.int32)],
        cost_estimate=pl.CostEstimate(flops=20_000_000, bytes_accessed=9_000_000, transcendentals=0),
        name="prepare",
    )(where, tiles, places, *weights)


def network_kernel(count, meta, state, after, *refs):
    given, (own, send, grads), kept = refs[:5], refs[5:8], refs[8:13]
    xbuf, abuf, slope1, slope2, sems, loads, leave = refs[13:]
    w1t, w2t, w2, w3t, w3 = kept
    total, core = meta[0], meta[1]
    steps = (total + STEP - 1) // STEP
    per_row = state.shape[2] // BW
    levels = w1t.shape[1]
    hid = w2.shape[0]
    groups = (meta.shape[0] - 2) // 2

    def copies(step, slot, i):
        spot = meta[2 + step * STEP + i]
        row, col = spot // per_row, pl.multiple_of((spot % per_row) * BW, BW)
        lanes = pl.ds(i * BW, BW)
        return (
            pltpu.make_async_copy(
                state.at[:, row, pl.ds(col, BW)], xbuf.at[slot, :, lanes], sems.at[slot, i, 0]
            ),
            pltpu.make_async_copy(
                after.at[:, row, pl.ds(col, BW)], abuf.at[slot, :, lanes], sems.at[slot, i, 1]
            ),
        )

    def fetch(step, slot):
        for i in range(STEP):

            @pl.when(step * STEP + i < total)
            def _():
                for copy in copies(step, slot, i):
                    copy.start()

    @pl.when(steps > 0)
    def _():
        fetch(0, 0)

    moves = [pltpu.make_async_copy(given[i], kept[i], loads.at[i]) for i in range(5)]
    for move in moves:
        move.start()
    grads[...] = jnp.zeros_like(grads)
    lane = lax.broadcasted_iota(jnp.int32, (1, STEP * BW), 1) // BW
    for move in moves:
        move.wait()

    def body(step, carry):
        slot = lax.rem(step, 2)

        @pl.when(step + 1 < steps)
        def _():
            fetch(step + 1, 1 - slot)

        for i in range(STEP):
            index = step * STEP + i

            @pl.when(index < total)
            def _():
                for copy in copies(step, slot, i):
                    copy.wait()

            @pl.when(index >= total)
            def _():
                zero = jnp.zeros((levels, BW), F32)
                xbuf[slot, :, i * BW : (i + 1) * BW] = zero
                abuf[slot, :, i * BW : (i + 1) * BW] = zero

        x = xbuf[slot]
        inputs = x.astype(BF16)
        targets = (TARGET_GAIN * (abuf[slot] - x)).astype(BF16)
        act_one, slope1[...] = activate(dot(w1t[...], inputs))
        act_two, slope2[...] = activate(dot(w2t[...], act_one))
        output = dot(w3t[...], act_two)
        times = jnp.ones((1, STEP * BW), F32)
        for i in range(STEP):
            index = step * STEP + i
            often = jnp.where(index < total, meta[2 + groups + jnp.minimum(index, groups - 1)], 1)
            times = jnp.where(lane == i, often.astype(F32), times)
        error = ((output - targets.astype(F32)) / count).astype(BF16)
        error = (error.astype(F32) * times).astype(BF16)
        grads[:, :, :, 72:] += dot_t(act_two, error).reshape(2, 8, 8, 8, BW)
        delta_two = (dot(w3[...], error) * slope2[...]).astype(BF16)
        for j in range(0, hid // BW, 2):
            both = dot_t(act_one, delta_two[j * BW : (j + 2) * BW])
            for k in (0, 1):
                at = (j + k) * 8
                grads[:, :, :, at : at + 8] += both[:, k * BW : (k + 1) * BW].reshape(2, 8, 8, 8, BW)
        delta_one = (dot(w2[...], delta_two) * slope1[...]).astype(BF16)
        for j in range(0, hid // BW, 2):
            both = dot_t(inputs, delta_one[j * BW : (j + 2) * BW])
            for k in (0, 1):
                grads[:, :, j + k, 64:72] += both[:, k * BW : (k + 1) * BW].reshape(2, 8, 8, BW)
        return carry

    lax.fori_loop(0, steps, body, 0)
    out = pltpu.make_async_copy(grads.at[core], own, leave)
    out.start()
    store_split(send, grads[1 - core].reshape(SHARDS, 80, BW))
    out.wait()


def network(meta, state, after, ready, count):
    hid, levels = ready[0].shape
    vmem = pl.BlockSpec(memory_space=pltpu.VMEM)
    hbm = pl.BlockSpec(memory_space=pl.ANY)
    width = STEP * BW
    return pl.pallas_call(
        functools.partial(network_kernel, count),
        out_shape=(
            jax.ShapeDtypeStruct((8, 8, 80, BW), F32),
            jax.ShapeDtypeStruct((SHARDS, 88, BW), BF16),
        ),
        in_specs=[pl.BlockSpec(memory_space=pltpu.SMEM)] + [hbm] * 7,
        out_specs=(hbm, vmem),
        scratch_shapes=[pltpu.VMEM((2, 8, 8, 80, BW), F32)]
        + [pltpu.VMEM(w.shape, BF16) for w in ready]
        + [
            pltpu.VMEM((2, levels, width), F32),
            pltpu.VMEM((2, levels, width), F32),
            pltpu.VMEM((hid, width), F32),
            pltpu.VMEM((hid, width), F32),
            pltpu.SemaphoreType.DMA((2, STEP, 2)),
            pltpu.SemaphoreType.DMA((5,)),
            pltpu.SemaphoreType.DMA,
        ],
        compiler_params=pltpu.CompilerParams(vmem_limit_bytes=56 * 1024 * 1024),
        name="network",
    )(meta, state, after, *ready)


def update_kernel(core, mine, theirs, w_in, w_mid, w_out, new_in, new_mid, new_out):
    for total, half in ((mine, core[0]), (theirs, 1 - core[0])):

        def part(a, carry, total=total, half=half):
            block = half * 8 + a
            for b in range(8):
                step = RATE * total[a, b]
                lanes = slice(b * BW, (b + 1) * BW)
                rows = pl.ds(pl.multiple_of(block * 8, 8), 8)
                new_in[rows, lanes] = w_in[rows, lanes] - step[64:72]
                rows = pl.ds(pl.multiple_of(block * 64 + b * 8, 8), 8)
                new_out[rows, :] = w_out[rows, :] - step[72:]
                for j in range(8):
                    lanes = slice(j * BW, (j + 1) * BW)
                    new_mid[rows, lanes] = w_mid[rows, lanes] - step[j * 8 : (j + 1) * 8]
            return carry

        lax.fori_loop(0, 8, part, 0)


def update(core, mine, theirs, weights):
    vmem = pl.BlockSpec(memory_space=pltpu.VMEM)
    return pl.pallas_call(
        update_kernel,
        out_shape=[jax.ShapeDtypeStruct(w.shape, F32) for w in weights],
        in_specs=[pl.BlockSpec(memory_space=pltpu.SMEM)] + [vmem] * 5,
        out_specs=[vmem] * 3,
        compiler_params=pltpu.CompilerParams(vmem_limit_bytes=24 * 1024 * 1024),
        name="update",
    )(core[None], mine, theirs, *weights)


def sum_everywhere(own, send, weights):
    core = lax.axis_index("c")
    swap = [(0, 1), (1, 0)]
    got = lax.ppermute(send, "c", swap).astype(F32)
    pair = own.reshape(SHARDS, 80, BW) + got[:, :80]
    last = pair[:, 72:] + got[:, 80:]
    high = lax.reduce_precision(last, 8, 7)
    pair = jnp.concatenate([pair[:, :72], high, last - high], axis=1).astype(BF16)
    ring, plane = lax.axis_size(RING), lax.axis_size(PLANE)
    held = lax.all_to_all(pair.reshape(-1, BW), PLANE, 0, 0, tiled=True)
    held = jnp.sum(held.reshape(plane, -1, BW).astype(F32), axis=0)
    held = held.reshape(ring, 88, BW)
    held = jnp.concatenate([held[:, :72], held[:, 72:80] + held[:, 80:]], axis=1).reshape(-1, BW)
    rows = held.shape[0]
    held = jnp.broadcast_to(held, (ring, rows, BW)).reshape(-1, BW)
    held = lax.all_to_all(held, RING, 0, 0, tiled=True)
    held = jnp.sum(held.reshape(ring, rows, BW), axis=0)
    power = jnp.floor(jnp.log2(jnp.maximum(jnp.max(jnp.abs(held)), 1e-30)))
    sent = (held * jnp.exp2(14.0 - power)).astype(jnp.float16)
    sent = jnp.concatenate([sent, jnp.full((8, BW), power, jnp.float16)])
    sent = jnp.broadcast_to(sent, (plane, rows + 8, BW)).reshape(-1, BW)
    sent = lax.all_to_all(sent, PLANE, 0, 0, tiled=True)
    away = lax.ppermute(sent, "c", swap)

    def opened(block):
        block = block.reshape(plane, rows + 8, BW).astype(F32)
        return (block[:, :rows] * jnp.exp2(block[:, rows : rows + 1] - 14.0)).reshape(8, 8, 80, BW)

    return update(core, opened(sent), opened(away), weights)


def on_device(state_field, diffusion, weight_in, weight_mid, weight_out, block_tile, block_pos):
    senders = lax.axis_size(SIM)
    samples = block_tile.shape[0] // senders
    _, tile_rows, tile_cols = state_field.shape
    weights = (weight_in, weight_mid, weight_out)
    where = jnp.stack([lax.axis_index(SIM), lax.axis_index("c")]).astype(jnp.int32)
    edges, late = exchange(state_field, (where, block_tile[:, 0], block_pos))
    meta, *ready = prepare(*late, weights, senders, tile_rows * tile_cols // BW)
    after = stencil_call(state_field, *edges(), diffusion)
    count = float(senders * lax.axis_size(LEARN) * samples * BW)
    own, send = network(meta, state_field, after, ready, count)
    new_in, new_mid, new_out = sum_everywhere(own, send, weights)
    return (after, new_in, new_mid, new_out)


def solution(mesh):
    fine = Mesh(mesh.devices.reshape(4, 4, 2, 2, 2), SIM + LEARN)
    placed = (P(None, SIM, LEARN), P(), P(), P(), P(), P(LEARN, None), P(LEARN))
    return jax.shard_map(
        on_device,
        mesh=fine,
        in_specs=placed,
        out_specs=(P(None, SIM, LEARN), P(), P(), P()),
        check_vma=False,
    )
```

```python
import functools

import jax
import jax.numpy as jnp
from jax import lax
from jax.experimental import pallas as pl
from jax.experimental.pallas import tpu as pltpu
from jax.sharding import Mesh
from jax.sharding import PartitionSpec as P


BW = 128
RATE = 0.5
TARGET_GAIN = 4.0
STEP = 4
SHARDS = 64

SIM = ("z", "y", "xh")
LEARN = ("xl", "c")
RING = ("xh", "xl")
PLANE = ("z", "y")

BF16 = jnp.bfloat16
F32 = jnp.float32


def shift(x, axis, by):
    size = lax.axis_size(axis)
    return lax.ppermute(x, axis, [(i, (i + by) % size) for i in range(size)])


GROUP = 8


def stencil_kernel(diffusion, tips, state, below, above, edge_cols, after, *held):
    chunk, rows, cols = state.shape
    base = pl.program_id(0) * chunk
    tall, wide = rows + 8, cols + BW
    fields, beside = held
    row = lax.broadcasted_iota(jnp.int32, (8, BW), 0)
    lane = lax.broadcasted_iota(jnp.int32, (8, BW), 1)
    gap = jnp.zeros((4, cols), F32)
    ends = [(at, spot) for at in (0, 7) for spot in (BW - 1, 0)]

    def sideways(field):
        return pltpu.roll(field, 1, 1) + pltpu.roll(field, wide - 1, 1)

    def diffuse(g, at):
        rate = diffusion[base + at]
        field = fields[g]
        around = pltpu.roll(field, 1, 0) + pltpu.roll(field, tall - 1, 0) + beside[g]
        return (1.0 - 4.0 * rate) * field + rate * around

    def group(index, carry):
        spots = [(g, index * GROUP + g) for g in range(GROUP)]
        for g, at in spots:
            upper = jnp.concatenate([state[at], edge_cols[at]], axis=1)
            corners = jnp.zeros((8, BW), F32)
            for tip, (end, spot) in enumerate(ends):
                corners = jnp.where((row == end) & (lane == spot), tips[tip, base + at], corners)
            lower = jnp.concatenate([below[at], gap, above[at]], axis=0)
            lower = jnp.concatenate([lower, corners], axis=1)
            field = jnp.concatenate([upper, lower], axis=0)
            fields[g] = field
            beside[g] = sideways(field)
        for g, at in spots:
            fields[g] = diffuse(g, at)
        for g, at in spots:
            beside[g] = sideways(fields[g])
        for g, at in spots:
            after[at] = diffuse(g, at)[:rows, :cols]
        return carry

    lax.fori_loop(0, chunk // GROUP, group, 0)


def exchange(state):
    levels, rows, cols = state.shape
    half = jnp.float16
    left = shift(jnp.transpose(state[:, :, cols - 2 :], (2, 1, 0)), LEARN, 1)
    right = shift(jnp.transpose(state[:, :, :2], (2, 1, 0)), LEARN, -1)

    def outgoing(first, at):
        ends = jnp.concatenate([left[1, at], right[0, at], jnp.zeros((cols - 2 * levels,), F32)])
        ends = jnp.stack([ends, jnp.zeros_like(ends)])[None]
        return jnp.concatenate([state[:, first : first + 2], ends]).astype(half)

    ends = (outgoing(rows - 2, rows - 1), outgoing(0, 0))
    above = shift(ends[0], SIM, 1)
    below = shift(ends[1], SIM, -1)

    def edges():
        edge_cols = jnp.concatenate([right, jnp.zeros((BW - 4, rows, levels), F32), left])
        edge_cols = jnp.transpose(edge_cols, (2, 1, 0))
        below_f32, above_f32 = below.astype(F32), above.astype(F32)
        tips = jnp.concatenate(
            [block[levels, 0, : 2 * levels].reshape(2, levels) for block in (below_f32, above_f32)]
        )
        return tips, below_f32, above_f32, edge_cols

    return edges


def stencil_call(state, tips, below, above, edge_cols, diffusion):
    levels, rows, cols = state.shape
    chunk = 32

    def block(*shape):
        return pl.BlockSpec((chunk,) + shape, lambda i: (i, 0, 0))

    smem = pl.BlockSpec(memory_space=pltpu.SMEM)
    return pl.pallas_call(
        stencil_kernel,
        out_shape=jax.ShapeDtypeStruct(state.shape, F32),
        grid=(levels // chunk,),
        in_specs=[smem, smem, block(rows, cols)]
        + [block(2, cols), block(2, cols), block(rows, BW)],
        out_specs=block(rows, cols),
        scratch_shapes=[pltpu.VMEM((GROUP, rows + 8, cols + BW), F32)] * 2,
        name="stencil",
    )(diffusion, tips, state, below, above, edge_cols)


def dot(a, b):
    return jnp.dot(a, b, preferred_element_type=F32)


def dot_t(a, b):
    return lax.dot_general(a, b, (((1,), (1,)), ((), ())), preferred_element_type=F32)


def activate(value):
    sigma = 0.5 * jnp.tanh(0.5 * value) + 0.5
    act = value * sigma
    return act.astype(BF16), sigma + act * (1.0 - sigma)


def store_split(target, block):
    high = block.astype(BF16)
    low = (block[:, 72:] - high[:, 72:].astype(F32)).astype(BF16)
    target[:, :80], target[:, 80:] = high, low


def prepare_kernel(where, tiles, places, w_in, w_mid, w_out, meta, w1t, w2t, w2, w3t, w3, held):
    w1t[...] = w_in[...].T.astype(BF16)
    w2t[...] = w_mid[...].T.astype(BF16)
    w2[...] = w_mid[...].astype(BF16)
    w3t[...] = w_out[...].T.astype(BF16)
    w3[...] = w_out[...].astype(BF16)
    groups = (meta.shape[0] - 2) // 2
    samples = tiles.shape[0] // groups

    def clear(i, carry):
        held[i] = 0
        return carry

    lax.fori_loop(0, held.shape[0], clear, 0)

    def group(g, count):
        place = -1
        for k in range(samples):
            place = jnp.where(tiles[g * samples + k] == where[0], places[g * samples + k], place)
        spot = jnp.maximum(place, 0)
        earlier = held[spot]
        fresh = (place >= 0) & (earlier == 0)

        @pl.when((place >= 0) & (earlier > 0))
        def _():
            at = 2 + groups + earlier - 1
            meta[at] = meta[at] + 1

        @pl.when(fresh)
        def _():
            meta[2 + count] = spot
            meta[2 + groups + count] = 1
            held[spot] = count + 1

        return count + fresh.astype(jnp.int32)

    meta[0] = lax.fori_loop(0, groups, group, 0)
    meta[1] = where[1]


def prepare(where, tiles, places, weights, groups, spots):
    levels, hid = weights[0].shape
    smem = pl.BlockSpec(memory_space=pltpu.SMEM)
    vmem = pl.BlockSpec(memory_space=pltpu.VMEM)
    shapes = ((hid, levels), (hid, hid), (hid, hid), (levels, hid), (hid, levels))
    return pl.pallas_call(
        prepare_kernel,
        out_shape=[jax.ShapeDtypeStruct((2 + 2 * groups,), jnp.int32)]
        + [jax.ShapeDtypeStruct(shape, BF16) for shape in shapes],
        in_specs=[smem] * 3 + [vmem] * 3,
        out_specs=[smem] + [vmem] * 5,
        scratch_shapes=[pltpu.SMEM((spots,), jnp.int32)],
        cost_estimate=pl.CostEstimate(flops=20_000_000, bytes_accessed=9_000_000, transcendentals=0),
        name="prepare",
    )(where, tiles, places, *weights)


def network_kernel(count, meta, state, after, *refs):
    given, (own, send, grads), kept = refs[:5], refs[5:8], refs[8:13]
    xbuf, abuf, slope1, slope2, sems, loads, leave = refs[13:]
    w1t, w2t, w2, w3t, w3 = kept
    total, core = meta[0], meta[1]
    steps = (total + STEP - 1) // STEP
    per_row = state.shape[2] // BW
    levels = w1t.shape[1]
    hid = w2.shape[0]
    groups = (meta.shape[0] - 2) // 2

    def copies(step, slot, i):
        spot = meta[2 + step * STEP + i]
        row, col = spot // per_row, pl.multiple_of((spot % per_row) * BW, BW)
        lanes = pl.ds(i * BW, BW)
        return (
            pltpu.make_async_copy(
                state.at[:, row, pl.ds(col, BW)], xbuf.at[slot, :, lanes], sems.at[slot, i, 0]
            ),
            pltpu.make_async_copy(
                after.at[:, row, pl.ds(col, BW)], abuf.at[slot, :, lanes], sems.at[slot, i, 1]
            ),
        )

    def fetch(step, slot):
        for i in range(STEP):

            @pl.when(step * STEP + i < total)
            def _():
                for copy in copies(step, slot, i):
                    copy.start()

    @pl.when(steps > 0)
    def _():
        fetch(0, 0)

    moves = [pltpu.make_async_copy(given[i], kept[i], loads.at[i]) for i in range(5)]
    for move in moves:
        move.start()
    grads[...] = jnp.zeros_like(grads)
    lane = lax.broadcasted_iota(jnp.int32, (1, STEP * BW), 1) // BW
    for move in moves:
        move.wait()

    def body(step, carry):
        slot = lax.rem(step, 2)

        @pl.when(step + 1 < steps)
        def _():
            fetch(step + 1, 1 - slot)

        for i in range(STEP):
            index = step * STEP + i

            @pl.when(index < total)
            def _():
                for copy in copies(step, slot, i):
                    copy.wait()

            @pl.when(index >= total)
            def _():
                zero = jnp.zeros((levels, BW), F32)
                xbuf[slot, :, i * BW : (i + 1) * BW] = zero
                abuf[slot, :, i * BW : (i + 1) * BW] = zero

        x = xbuf[slot]
        inputs = x.astype(BF16)
        targets = (TARGET_GAIN * (abuf[slot] - x)).astype(BF16)
        act_one, slope1[...] = activate(dot(w1t[...], inputs))
        act_two, slope2[...] = activate(dot(w2t[...], act_one))
        output = dot(w3t[...], act_two)
        times = jnp.ones((1, STEP * BW), F32)
        for i in range(STEP):
            index = step * STEP + i
            often = jnp.where(index < total, meta[2 + groups + jnp.minimum(index, groups - 1)], 1)
            times = jnp.where(lane == i, often.astype(F32), times)
        error = ((output - targets.astype(F32)) / count).astype(BF16)
        error = (error.astype(F32) * times).astype(BF16)
        grads[:, :, :, 72:] += dot_t(act_two, error).reshape(2, 8, 8, 8, BW)
        delta_two = (dot(w3[...], error) * slope2[...]).astype(BF16)
        for j in range(0, hid // BW, 2):
            both = dot_t(act_one, delta_two[j * BW : (j + 2) * BW])
            for k in (0, 1):
                at = (j + k) * 8
                grads[:, :, :, at : at + 8] += both[:, k * BW : (k + 1) * BW].reshape(2, 8, 8, 8, BW)
        delta_one = (dot(w2[...], delta_two) * slope1[...]).astype(BF16)
        for j in range(0, hid // BW, 2):
            both = dot_t(inputs, delta_one[j * BW : (j + 2) * BW])
            for k in (0, 1):
                grads[:, :, j + k, 64:72] += both[:, k * BW : (k + 1) * BW].reshape(2, 8, 8, BW)
        return carry

    lax.fori_loop(0, steps, body, 0)
    out = pltpu.make_async_copy(grads.at[core], own, leave)
    out.start()
    store_split(send, grads[1 - core].reshape(SHARDS, 80, BW))
    out.wait()


def network(meta, state, after, ready, count):
    hid, levels = ready[0].shape
    vmem = pl.BlockSpec(memory_space=pltpu.VMEM)
    hbm = pl.BlockSpec(memory_space=pl.ANY)
    width = STEP * BW
    return pl.pallas_call(
        functools.partial(network_kernel, count),
        out_shape=(
            jax.ShapeDtypeStruct((8, 8, 80, BW), F32),
            jax.ShapeDtypeStruct((SHARDS, 88, BW), BF16),
        ),
        in_specs=[pl.BlockSpec(memory_space=pltpu.SMEM)] + [hbm] * 7,
        out_specs=(hbm, vmem),
        scratch_shapes=[pltpu.VMEM((2, 8, 8, 80, BW), F32)]
        + [pltpu.VMEM(w.shape, BF16) for w in ready]
        + [
            pltpu.VMEM((2, levels, width), F32),
            pltpu.VMEM((2, levels, width), F32),
            pltpu.VMEM((hid, width), F32),
            pltpu.VMEM((hid, width), F32),
            pltpu.SemaphoreType.DMA((2, STEP, 2)),
            pltpu.SemaphoreType.DMA((5,)),
            pltpu.SemaphoreType.DMA,
        ],
        compiler_params=pltpu.CompilerParams(vmem_limit_bytes=56 * 1024 * 1024),
        name="network",
    )(meta, state, after, *ready)


PIECES = 2


def update_kernel(core, mine, theirs, *refs):
    weights, news, held, stores = refs[:3], refs[3:6], refs[6:9], refs[9]
    span = 8 // PIECES
    moves = []
    for order, (total, half) in enumerate(((mine, core[0]), (theirs, 1 - core[0]))):
        for piece in range(PIECES):

            def rows_of(i, first, count, half=half, piece=piece):
                size = weights[i].shape[0] // (2 * PIECES)
                start = (half * PIECES + piece) * size + first
                return pl.ds(pl.multiple_of(start, 8), count)

            for a in range(span):
                for b in range(8):
                    step = RATE * total[piece * span + a, b]
                    lanes = slice(b * BW, (b + 1) * BW)
                    old = weights[0][rows_of(0, a * 8, 8), lanes]
                    held[0][order, piece, a * 8 : (a + 1) * 8, lanes] = old - step[64:72]
                    at = a * 64 + b * 8
                    old = weights[2][rows_of(2, at, 8), :]
                    held[2][order, piece, at : at + 8] = old - step[72:]
                    for j in range(8):
                        lanes = slice(j * BW, (j + 1) * BW)
                        old = weights[1][rows_of(1, at, 8), lanes]
                        held[1][order, piece, at : at + 8, lanes] = old - step[j * 8 : (j + 1) * 8]
            for i in range(3):
                target = news[i].at[rows_of(i, 0, held[i].shape[2])]
                move = pltpu.make_async_copy(
                    held[i].at[order, piece], target, stores.at[order * PIECES + piece, i]
                )
                move.start()
                moves.append(move)
    for move in moves:
        move.wait()


def update(core, mine, theirs, weights):
    vmem = pl.BlockSpec(memory_space=pltpu.VMEM)
    return pl.pallas_call(
        update_kernel,
        out_shape=[jax.ShapeDtypeStruct(w.shape, F32) for w in weights],
        in_specs=[pl.BlockSpec(memory_space=pltpu.SMEM)] + [vmem] * 5,
        out_specs=[pl.BlockSpec(memory_space=pl.ANY)] * 3,
        scratch_shapes=[
            pltpu.VMEM((2, PIECES, w.shape[0] // (2 * PIECES), w.shape[1]), F32) for w in weights
        ]
        + [pltpu.SemaphoreType.DMA((2 * PIECES, 3))],
        compiler_params=pltpu.CompilerParams(vmem_limit_bytes=24 * 1024 * 1024),
        name="update",
    )(core[None], mine, theirs, *weights)


def sum_everywhere(own, send, weights):
    core = lax.axis_index("c")
    swap = [(0, 1), (1, 0)]
    got = lax.ppermute(send, "c", swap).astype(F32)
    pair = own.reshape(SHARDS, 80, BW) + got[:, :80]
    last = pair[:, 72:] + got[:, 80:]
    high = lax.reduce_precision(last, 8, 7)
    pair = jnp.concatenate([pair[:, :72], high, last - high], axis=1).astype(BF16)
    ring, plane = lax.axis_size(RING), lax.axis_size(PLANE)
    held = lax.all_to_all(pair.reshape(-1, BW), PLANE, 0, 0, tiled=True)
    held = jnp.sum(held.reshape(plane, -1, BW).astype(F32), axis=0)
    held = held.reshape(ring, 88, BW)
    held = jnp.concatenate([held[:, :72], held[:, 72:80] + held[:, 80:]], axis=1).reshape(-1, BW)
    rows = held.shape[0]
    held = jnp.broadcast_to(held, (ring, rows, BW)).reshape(-1, BW)
    held = lax.all_to_all(held, RING, 0, 0, tiled=True)
    held = jnp.sum(held.reshape(ring, rows, BW), axis=0)
    power = jnp.floor(jnp.log2(jnp.maximum(jnp.max(jnp.abs(held)), 1e-30)))
    sent = (held * jnp.exp2(14.0 - power)).astype(jnp.float16)
    sent = jnp.concatenate([sent, jnp.full((8, BW), power, jnp.float16)])
    sent = jnp.broadcast_to(sent, (plane, rows + 8, BW)).reshape(-1, BW)
    sent = lax.all_to_all(sent, PLANE, 0, 0, tiled=True)
    away = lax.ppermute(sent, "c", swap)

    def opened(block):
        block = block.reshape(plane, rows + 8, BW).astype(F32)
        return (block[:, :rows] * jnp.exp2(block[:, rows : rows + 1] - 14.0)).reshape(8, 8, 80, BW)

    return update(core, opened(sent), opened(away), weights)


def on_device(state_field, diffusion, weight_in, weight_mid, weight_out, block_tile, block_pos):
    senders = lax.axis_size(SIM)
    samples = block_tile.shape[0] // senders
    _, tile_rows, tile_cols = state_field.shape
    weights = (weight_in, weight_mid, weight_out)
    where = jnp.stack([lax.axis_index(SIM), lax.axis_index("c")]).astype(jnp.int32)
    edges = exchange(state_field)
    spots = tile_rows * tile_cols // BW
    meta, *ready = prepare(where, block_tile[:, 0], block_pos, weights, senders, spots)
    after = stencil_call(state_field, *edges(), diffusion)
    count = float(senders * lax.axis_size(LEARN) * samples * BW)
    own, send = network(meta, state_field, after, ready, count)
    new_in, new_mid, new_out = sum_everywhere(own, send, weights)
    return (after, new_in, new_mid, new_out)


def solution(mesh):
    fine = Mesh(mesh.devices.reshape(4, 4, 2, 2, 2), SIM + LEARN)
    placed = (P(None, SIM, LEARN), P(), P(), P(), P(), P(LEARN, None), P(LEARN))
    return jax.shard_map(
        on_device,
        mesh=fine,
        in_specs=placed,
        out_specs=(P(None, SIM, LEARN), P(), P(), P()),
        check_vma=False,
    )
```

```python
import functools

import jax
import jax.numpy as jnp
from jax import lax
from jax.experimental import pallas as pl
from jax.experimental.pallas import tpu as pltpu
from jax.sharding import Mesh
from jax.sharding import PartitionSpec as P


BW = 128
RATE = 0.5
TARGET_GAIN = 4.0
STEP = 4
SHARDS = 64

SIM = ("z", "y", "xh")
LEARN = ("xl", "c")
RING = ("xh", "xl")
PLANE = ("z", "y")

BF16 = jnp.bfloat16
F32 = jnp.float32


def shift(x, axis, by):
    size = lax.axis_size(axis)
    return lax.ppermute(x, axis, [(i, (i + by) % size) for i in range(size)])


GROUP = 8


def stencil_kernel(diffusion, tips, state, below, above, edge_cols, after, *held):
    chunk, rows, cols = state.shape
    base = pl.program_id(0) * chunk
    tall, wide = rows + 8, cols + BW
    fields, beside = held
    row = lax.broadcasted_iota(jnp.int32, (8, BW), 0)
    lane = lax.broadcasted_iota(jnp.int32, (8, BW), 1)
    gap = jnp.zeros((4, cols), F32)
    ends = [(at, spot) for at in (0, 7) for spot in (BW - 1, 0)]

    def sideways(field):
        return pltpu.roll(field, 1, 1) + pltpu.roll(field, wide - 1, 1)

    def diffuse(g, at):
        rate = diffusion[base + at]
        field = fields[g]
        around = pltpu.roll(field, 1, 0) + pltpu.roll(field, tall - 1, 0) + beside[g]
        return (1.0 - 4.0 * rate) * field + rate * around

    def group(index, carry):
        spots = [(g, index * GROUP + g) for g in range(GROUP)]
        for g, at in spots:
            upper = jnp.concatenate([state[at], edge_cols[at]], axis=1)
            corners = jnp.zeros((8, BW), F32)
            for tip, (end, spot) in enumerate(ends):
                corners = jnp.where((row == end) & (lane == spot), tips[tip, base + at], corners)
            lower = jnp.concatenate([below[at], gap, above[at]], axis=0)
            lower = jnp.concatenate([lower, corners], axis=1)
            field = jnp.concatenate([upper, lower], axis=0)
            fields[g] = field
            beside[g] = sideways(field)
        for g, at in spots:
            fields[g] = diffuse(g, at)
        for g, at in spots:
            beside[g] = sideways(fields[g])
        for g, at in spots:
            after[at] = diffuse(g, at)[:rows, :cols]
        return carry

    lax.fori_loop(0, chunk // GROUP, group, 0)


def exchange(state):
    levels, rows, cols = state.shape
    half = jnp.float16
    left = shift(jnp.transpose(state[:, :, cols - 2 :], (2, 1, 0)), LEARN, 1)
    right = shift(jnp.transpose(state[:, :, :2], (2, 1, 0)), LEARN, -1)

    def outgoing(first, at):
        ends = jnp.concatenate([left[1, at], right[0, at], jnp.zeros((cols - 2 * levels,), F32)])
        ends = jnp.stack([ends, jnp.zeros_like(ends)])[None]
        return jnp.concatenate([state[:, first : first + 2], ends]).astype(half)

    ends = (outgoing(rows - 2, rows - 1), outgoing(0, 0))
    above = shift(ends[0], SIM, 1)
    below = shift(ends[1], SIM, -1)

    def edges():
        edge_cols = jnp.concatenate([right, jnp.zeros((BW - 4, rows, levels), F32), left])
        edge_cols = jnp.transpose(edge_cols, (2, 1, 0))
        below_f32, above_f32 = below.astype(F32), above.astype(F32)
        tips = jnp.concatenate(
            [block[levels, 0, : 2 * levels].reshape(2, levels) for block in (below_f32, above_f32)]
        )
        return tips, below_f32, above_f32, edge_cols

    return edges


def stencil_call(state, tips, below, above, edge_cols, diffusion):
    levels, rows, cols = state.shape
    chunk = 32

    def block(*shape):
        return pl.BlockSpec((chunk,) + shape, lambda i: (i, 0, 0))

    smem = pl.BlockSpec(memory_space=pltpu.SMEM)
    return pl.pallas_call(
        stencil_kernel,
        out_shape=jax.ShapeDtypeStruct(state.shape, F32),
        grid=(levels // chunk,),
        in_specs=[smem, smem, block(rows, cols)]
        + [block(2, cols), block(2, cols), block(rows, BW)],
        out_specs=block(rows, cols),
        scratch_shapes=[pltpu.VMEM((GROUP, rows + 8, cols + BW), F32)] * 2,
        name="stencil",
    )(diffusion, tips, state, below, above, edge_cols)


def dot(a, b):
    return jnp.dot(a, b, preferred_element_type=F32)


def dot_t(a, b):
    return lax.dot_general(a, b, (((1,), (1,)), ((), ())), preferred_element_type=F32)


def activate(value):
    sigma = 0.5 * jnp.tanh(0.5 * value) + 0.5
    act = value * sigma
    return act.astype(BF16), sigma + act * (1.0 - sigma)


def store_split(target, block):
    high = block.astype(BF16)
    low = (block[:, 72:] - high[:, 72:].astype(F32)).astype(BF16)
    target[:, :80], target[:, 80:] = high, low


def prepare_kernel(where, tiles, places, w_in, w_mid, w_out, meta, w1t, w2t, w2, w3t, w3, held):
    w1t[...] = w_in[...].T.astype(BF16)
    w2t[...] = w_mid[...].T.astype(BF16)
    w2[...] = w_mid[...].astype(BF16)
    w3t[...] = w_out[...].T.astype(BF16)
    w3[...] = w_out[...].astype(BF16)
    groups = (meta.shape[0] - 2) // 2
    samples = tiles.shape[0] // groups

    def clear(i, carry):
        held[i] = 0
        return carry

    lax.fori_loop(0, held.shape[0], clear, 0)

    def group(g, count):
        place = -1
        for k in range(samples):
            place = jnp.where(tiles[g * samples + k] == where[0], places[g * samples + k], place)
        spot = jnp.maximum(place, 0)
        earlier = held[spot]
        fresh = (place >= 0) & (earlier == 0)

        @pl.when((place >= 0) & (earlier > 0))
        def _():
            at = 2 + groups + earlier - 1
            meta[at] = meta[at] + 1

        @pl.when(fresh)
        def _():
            meta[2 + count] = spot
            meta[2 + groups + count] = 1
            held[spot] = count + 1

        return count + fresh.astype(jnp.int32)

    meta[0] = lax.fori_loop(0, groups, group, 0)
    meta[1] = where[1]


def prepare(where, tiles, places, weights, groups, spots):
    levels, hid = weights[0].shape
    smem = pl.BlockSpec(memory_space=pltpu.SMEM)
    vmem = pl.BlockSpec(memory_space=pltpu.VMEM)
    shapes = ((hid, levels), (hid, hid), (hid, hid), (levels, hid), (hid, levels))
    return pl.pallas_call(
        prepare_kernel,
        out_shape=[jax.ShapeDtypeStruct((2 + 2 * groups,), jnp.int32)]
        + [jax.ShapeDtypeStruct(shape, BF16) for shape in shapes],
        in_specs=[smem] * 3 + [vmem] * 3,
        out_specs=[smem] + [vmem] * 5,
        scratch_shapes=[pltpu.SMEM((spots,), jnp.int32)],
        cost_estimate=pl.CostEstimate(flops=20_000_000, bytes_accessed=9_000_000, transcendentals=0),
        name="prepare",
    )(where, tiles, places, *weights)


def network_kernel(count, meta, state, after, *refs):
    given, (own, send, grads), kept = refs[:5], refs[5:8], refs[8:13]
    xbuf, abuf, slope1, slope2, sems, loads, leave = refs[13:]
    w1t, w2t, w2, w3t, w3 = kept
    total, core = meta[0], meta[1]
    steps = (total + STEP // 2 - 1) // STEP
    per_row = state.shape[2] // BW
    levels = w1t.shape[1]
    hid = w2.shape[0]
    groups = (meta.shape[0] - 2) // 2

    def copies(step, slot, i):
        spot = meta[2 + step * STEP + i]
        row, col = spot // per_row, pl.multiple_of((spot % per_row) * BW, BW)
        lanes = pl.ds(i * BW, BW)
        return (
            pltpu.make_async_copy(
                state.at[:, row, pl.ds(col, BW)], xbuf.at[slot, :, lanes], sems.at[slot, i, 0]
            ),
            pltpu.make_async_copy(
                after.at[:, row, pl.ds(col, BW)], abuf.at[slot, :, lanes], sems.at[slot, i, 1]
            ),
        )

    def fetch(step, slot):
        for i in range(STEP):

            @pl.when(step * STEP + i < total)
            def _():
                for copy in copies(step, slot, i):
                    copy.start()

    fetch(0, 0)

    moves = [pltpu.make_async_copy(given[i], kept[i], loads.at[i]) for i in range(5)]
    for move in moves:
        move.start()
    grads[...] = jnp.zeros_like(grads)
    for move in moves:
        move.wait()

    def body(step, carry):
        fetch(step + 1, 1 - lax.rem(step, 2))
        learn(step, STEP)
        return carry

    def learn(step, blocks):
        slot = lax.rem(step, 2)
        width = blocks * BW
        lane = lax.broadcasted_iota(jnp.int32, (1, width), 1) // BW
        for i in range(blocks):
            index = step * STEP + i

            @pl.when(index < total)
            def _():
                for copy in copies(step, slot, i):
                    copy.wait()

            @pl.when(index >= total)
            def _():
                zero = jnp.zeros((levels, BW), F32)
                xbuf[slot, :, i * BW : (i + 1) * BW] = zero
                abuf[slot, :, i * BW : (i + 1) * BW] = zero

        x = xbuf[slot, :, :width]
        inputs = x.astype(BF16)
        targets = (TARGET_GAIN * (abuf[slot, :, :width] - x)).astype(BF16)
        act_one, slope1[:, :width] = activate(dot(w1t[...], inputs))
        act_two, slope2[:, :width] = activate(dot(w2t[...], act_one))
        output = dot(w3t[...], act_two)
        times = jnp.ones((1, width), F32)
        for i in range(blocks):
            index = step * STEP + i
            often = jnp.where(index < total, meta[2 + groups + jnp.minimum(index, groups - 1)], 1)
            times = jnp.where(lane == i, often.astype(F32), times)
        error = ((output - targets.astype(F32)) / count).astype(BF16)
        error = (error.astype(F32) * times).astype(BF16)
        grads[:, :, :, 72:] += dot_t(act_two, error).reshape(2, 8, 8, 8, BW)
        delta_two = (dot(w3[...], error) * slope2[:, :width]).astype(BF16)
        for j in range(0, hid // BW, 2):
            both = dot_t(act_one, delta_two[j * BW : (j + 2) * BW])
            for k in (0, 1):
                at = (j + k) * 8
                grads[:, :, :, at : at + 8] += both[:, k * BW : (k + 1) * BW].reshape(2, 8, 8, 8, BW)
        delta_one = (dot(w2[...], delta_two) * slope1[:, :width]).astype(BF16)
        for j in range(0, hid // BW, 2):
            both = dot_t(inputs, delta_one[j * BW : (j + 2) * BW])
            for k in (0, 1):
                grads[:, :, j + k, 64:72] += both[:, k * BW : (k + 1) * BW].reshape(2, 8, 8, BW)

    lax.fori_loop(0, steps, body, 0)

    @pl.when(steps * STEP < total)
    def _():
        learn(steps, STEP // 2)

    out = pltpu.make_async_copy(grads.at[core], own, leave)
    out.start()
    store_split(send, grads[1 - core].reshape(SHARDS, 80, BW))
    out.wait()


def network(meta, state, after, ready, count):
    hid, levels = ready[0].shape
    vmem = pl.BlockSpec(memory_space=pltpu.VMEM)
    hbm = pl.BlockSpec(memory_space=pl.ANY)
    width = STEP * BW
    return pl.pallas_call(
        functools.partial(network_kernel, count),
        out_shape=(
            jax.ShapeDtypeStruct((8, 8, 80, BW), F32),
            jax.ShapeDtypeStruct((SHARDS, 88, BW), BF16),
        ),
        in_specs=[pl.BlockSpec(memory_space=pltpu.SMEM)] + [hbm] * 7,
        out_specs=(hbm, vmem),
        scratch_shapes=[pltpu.VMEM((2, 8, 8, 80, BW), F32)]
        + [pltpu.VMEM(w.shape, BF16) for w in ready]
        + [
            pltpu.VMEM((2, levels, width), F32),
            pltpu.VMEM((2, levels, width), F32),
            pltpu.VMEM((hid, width), F32),
            pltpu.VMEM((hid, width), F32),
            pltpu.SemaphoreType.DMA((2, STEP, 2)),
            pltpu.SemaphoreType.DMA((5,)),
            pltpu.SemaphoreType.DMA,
        ],
        compiler_params=pltpu.CompilerParams(vmem_limit_bytes=56 * 1024 * 1024),
        name="network",
    )(meta, state, after, *ready)


PIECES = 2


def update_kernel(core, mine, theirs, *refs):
    weights, news, held, stores = refs[:3], refs[3:6], refs[6:9], refs[9]
    span = 8 // PIECES
    moves = []
    for order, (total, half) in enumerate(((mine, core[0]), (theirs, 1 - core[0]))):
        for piece in range(PIECES):

            def rows_of(i, first, count, half=half, piece=piece):
                size = weights[i].shape[0] // (2 * PIECES)
                start = (half * PIECES + piece) * size + first
                return pl.ds(pl.multiple_of(start, 8), count)

            for a in range(span):
                for b in range(8):
                    step = RATE * total[piece * span + a, b]
                    lanes = slice(b * BW, (b + 1) * BW)
                    old = weights[0][rows_of(0, a * 8, 8), lanes]
                    held[0][order, piece, a * 8 : (a + 1) * 8, lanes] = old - step[64:72]
                    at = a * 64 + b * 8
                    old = weights[2][rows_of(2, at, 8), :]
                    held[2][order, piece, at : at + 8] = old - step[72:]
                    for j in range(8):
                        lanes = slice(j * BW, (j + 1) * BW)
                        old = weights[1][rows_of(1, at, 8), lanes]
                        held[1][order, piece, at : at + 8, lanes] = old - step[j * 8 : (j + 1) * 8]
            for i in range(3):
                target = news[i].at[rows_of(i, 0, held[i].shape[2])]
                move = pltpu.make_async_copy(
                    held[i].at[order, piece], target, stores.at[order * PIECES + piece, i]
                )
                move.start()
                moves.append(move)
    for move in moves:
        move.wait()


def update(core, mine, theirs, weights):
    vmem = pl.BlockSpec(memory_space=pltpu.VMEM)
    return pl.pallas_call(
        update_kernel,
        out_shape=[jax.ShapeDtypeStruct(w.shape, F32) for w in weights],
        in_specs=[pl.BlockSpec(memory_space=pltpu.SMEM)] + [vmem] * 5,
        out_specs=[pl.BlockSpec(memory_space=pl.ANY)] * 3,
        scratch_shapes=[
            pltpu.VMEM((2, PIECES, w.shape[0] // (2 * PIECES), w.shape[1]), F32) for w in weights
        ]
        + [pltpu.SemaphoreType.DMA((2 * PIECES, 3))],
        compiler_params=pltpu.CompilerParams(vmem_limit_bytes=24 * 1024 * 1024),
        name="update",
    )(core[None], mine, theirs, *weights)


def sum_everywhere(own, send, weights):
    core = lax.axis_index("c")
    swap = [(0, 1), (1, 0)]
    got = lax.ppermute(send, "c", swap).astype(F32)
    pair = own.reshape(SHARDS, 80, BW) + got[:, :80]
    last = pair[:, 72:] + got[:, 80:]
    high = lax.reduce_precision(last, 8, 7)
    pair = jnp.concatenate([pair[:, :72], high, last - high], axis=1).astype(BF16)
    ring, plane = lax.axis_size(RING), lax.axis_size(PLANE)
    held = lax.all_to_all(pair.reshape(-1, BW), PLANE, 0, 0, tiled=True)
    held = jnp.sum(held.reshape(plane, -1, BW).astype(F32), axis=0)
    held = held.reshape(ring, 88, BW)
    held = jnp.concatenate([held[:, :72], held[:, 72:80] + held[:, 80:]], axis=1).reshape(-1, BW)
    rows = held.shape[0]
    held = jnp.broadcast_to(held, (ring, rows, BW)).reshape(-1, BW)
    held = lax.all_to_all(held, RING, 0, 0, tiled=True)
    held = jnp.sum(held.reshape(ring, rows, BW), axis=0)
    power = jnp.floor(jnp.log2(jnp.maximum(jnp.max(jnp.abs(held)), 1e-30)))
    sent = (held * jnp.exp2(14.0 - power)).astype(jnp.float16)
    sent = jnp.concatenate([sent, jnp.full((8, BW), power, jnp.float16)])
    sent = jnp.broadcast_to(sent, (plane, rows + 8, BW)).reshape(-1, BW)
    sent = lax.all_to_all(sent, PLANE, 0, 0, tiled=True)
    away = lax.ppermute(sent, "c", swap)

    def opened(block):
        block = block.reshape(plane, rows + 8, BW).astype(F32)
        return (block[:, :rows] * jnp.exp2(block[:, rows : rows + 1] - 14.0)).reshape(8, 8, 80, BW)

    return update(core, opened(sent), opened(away), weights)


def on_device(state_field, diffusion, weight_in, weight_mid, weight_out, block_tile, block_pos):
    senders = lax.axis_size(SIM)
    samples = block_tile.shape[0] // senders
    _, tile_rows, tile_cols = state_field.shape
    weights = (weight_in, weight_mid, weight_out)
    where = jnp.stack([lax.axis_index(SIM), lax.axis_index("c")]).astype(jnp.int32)
    edges = exchange(state_field)
    spots = tile_rows * tile_cols // BW
    meta, *ready = prepare(where, block_tile[:, 0], block_pos, weights, senders, spots)
    after = stencil_call(state_field, *edges(), diffusion)
    count = float(senders * lax.axis_size(LEARN) * samples * BW)
    own, send = network(meta, state_field, after, ready, count)
    new_in, new_mid, new_out = sum_everywhere(own, send, weights)
    return (after, new_in, new_mid, new_out)


def solution(mesh):
    fine = Mesh(mesh.devices.reshape(4, 4, 2, 2, 2), SIM + LEARN)
    placed = (P(None, SIM, LEARN), P(), P(), P(), P(), P(LEARN, None), P(LEARN))
    return jax.shard_map(
        on_device,
        mesh=fine,
        in_specs=placed,
        out_specs=(P(None, SIM, LEARN), P(), P(), P()),
        check_vma=False,
    )
```
